16 devices in a mesh: tp: 16 (over z, y, x, core).
Axes of the slice: x: 2, y: 2, z: 2, core: 2. Of those that a mesh axis runs over, the one named last changes fastest.
Arguments:
- x_norm: bfloat16 [1024, 2560], P(None, 'tp')
- hid_act: bfloat16 [1024, 6720], P(None, 'tp')
- dy_in: bfloat16 [2, 1024, 6720], replicated
- dy_out: bfloat16 [1024, 2560], replicated
- w_in: float32 [2, 2560, 6720], P(None, 'tp')
- w_out: float32 [6720, 2560], P('tp')
- row_in: float32 [2, 2560], P(None, 'tp')
- col_in: float32 [2, 6720], replicated
- row_out: float32 [6720], P('tp')
- col_out: float32 [2560], replicated
- beta_two: float32 [], replicated
- rel_step: float32 [], replicated
- clip_rms: float32 [], replicated
- clip_norm: float32 [], replicated
Outputs:
- output 1: float32 [2, 2560, 6720], P(None, 'tp')
- output 2: float32 [2, 2560], P(None, 'tp')
- output 3: float32 [2, 6720], replicated
- output 4: float32 [6720, 2560], P('tp')
- output 5: float32 [6720], P('tp')
- output 6: float32 [2560], replicated
All inputs are finite; a program needn't handle non-finite values.
Results may differ from the reference program's by a relative error of at most 0.001.
Values are sent between devices in bfloat16 or wider.
A program may use at most 1 GiB of HBM per device.

```python
import jax
import jax.numpy as jnp
from jax import lax

D = 2560
FF = 6720
TOK_DEV = 64
GROUP = 16
TOKENS = TOK_DEV * GROUP
EPS_ONE = 1e-30
EPS_TWO = 1e-3


def setup_inputs(seed: int = 0) -> dict:
    key_list = jax.random.split(jax.random.key(seed), 14)
    x_norm = jax.random.normal(key_list[0], (TOKENS, D), jnp.float32).astype(jnp.bfloat16)
    hid_act = jax.random.normal(key_list[1], (TOKENS, FF), jnp.float32).astype(jnp.bfloat16)
    dy_in = jax.random.normal(key_list[2], (2, TOKENS, FF), jnp.float32).astype(jnp.bfloat16)
    dy_out = jax.random.normal(key_list[3], (TOKENS, D), jnp.float32).astype(jnp.bfloat16)
    w_in = jax.random.normal(key_list[4], (2, D, FF), jnp.float32) * (D ** -0.5)
    w_out = jax.random.normal(key_list[5], (FF, D), jnp.float32) * (FF ** -0.5)
    stat_level = 0.2 * TOKENS
    row_in = stat_level * jax.random.uniform(key_list[6], (2, D), jnp.float32, minval=0.3, maxval=1.7)
    col_in = stat_level * jax.random.uniform(key_list[7], (2, FF), jnp.float32, minval=0.3, maxval=1.7)
    row_out = stat_level * jax.random.uniform(key_list[8], (FF,), jnp.float32, minval=0.3, maxval=1.7)
    col_out = stat_level * jax.random.uniform(key_list[9], (D,), jnp.float32, minval=0.3, maxval=1.7)
    beta_two = jax.random.uniform(key_list[10], (), jnp.float32, minval=0.5, maxval=0.9)
    rel_step = jax.random.uniform(key_list[11], (), jnp.float32, minval=0.2, maxval=0.8)
    clip_rms = jax.random.uniform(key_list[12], (), jnp.float32, minval=0.2, maxval=0.4)
    clip_frac = jax.random.uniform(key_list[13], (), jnp.float32, minval=0.35, maxval=0.6)
    clip_norm = clip_frac * (3.0 * TOKENS * D * FF) ** 0.5
    return {"x_norm": x_norm, "hid_act": hid_act, "dy_in": dy_in, "dy_out": dy_out,
            "w_in": w_in, "w_out": w_out, "row_in": row_in, "col_in": col_in,
            "row_out": row_out, "col_out": col_out, "beta_two": beta_two,
            "rel_step": rel_step, "clip_rms": clip_rms, "clip_norm": clip_norm}


def adafactor_update(weight, gradient, row_stat, col_stat, beta_two, rel_step, clip_rms, grad_scale):
    scaled = grad_scale * gradient
    sq_grad = scaled * scaled + EPS_ONE
    mix_new = 1.0 - beta_two
    row_new = beta_two * row_stat + mix_new * jnp.mean(sq_grad, axis=-1)
    col_new = beta_two * col_stat + mix_new * jnp.mean(sq_grad, axis=-2)
    row_level = jnp.mean(row_new, axis=-1, keepdims=True)
    second = (row_new / row_level)[..., :, None] * col_new[..., None, :]
    update = scaled / jnp.sqrt(second)
    upd_rms = jnp.sqrt(jnp.mean(update * update, axis=(-2, -1), keepdims=True))
    clipped = update / jnp.maximum(1.0, upd_rms / clip_rms)
    w_rms = jnp.sqrt(jnp.mean(weight * weight, axis=(-2, -1), keepdims=True))
    step_size = rel_step * jnp.maximum(EPS_TWO, w_rms)
    return weight - step_size * clipped, row_new, col_new


def reference(x_norm, hid_act, dy_in, dy_out, w_in, w_out, row_in, col_in, row_out, col_out, beta_two, rel_step, clip_rms, clip_norm):
    def input_grad(dy_one):
        return jnp.dot(x_norm.T, dy_one, preferred_element_type=jnp.float32)
    grad_in = lax.map(input_grad, dy_in)
    grad_out = jnp.dot(hid_act.T, dy_out, preferred_element_type=jnp.float32)
    norm_sq = jnp.sum(grad_in * grad_in) + jnp.sum(grad_out * grad_out)
    grad_scale = jnp.minimum(1.0, clip_norm / jnp.sqrt(norm_sq))
    new_in = adafactor_update(w_in, grad_in, row_in, col_in, beta_two, rel_step, clip_rms, grad_scale)
    new_out = adafactor_update(w_out, grad_out, row_out, col_out, beta_two, rel_step, clip_rms, grad_scale)
    return (new_in[0], new_in[1], new_in[2], new_out[0], new_out[1], new_out[2])
```

```python
import jax
import jax.numpy as jnp
from jax import lax
from jax.experimental import pallas as pl
from jax.experimental.pallas import tpu as pltpu
from jax.sharding import PartitionSpec as P

EPS_ONE = 1e-30
EPS_TWO = 1e-3
LANES = 128
F32 = jnp.float32
BF16 = jnp.bfloat16

OUT_ROW, IN_ROW, IN_STEP, STAT_ROWS = 0, 32, 64, 160
SCALAR_ROW = 24
GROUPS = ((0, 32), (32, 32), (64, 32), (128, 32), (96, 16), (112, 16))
CHUNK = 512
SUPER = 2048
SLOTS = 2


def lane_to_column(vec, rows):
    n = vec.shape[1]
    r = lax.broadcasted_iota(jnp.int32, (rows, n), 0)
    c = lax.broadcasted_iota(jnp.int32, (rows, n), 1)
    col = jnp.sum(jnp.where(r == c, jnp.broadcast_to(vec, (rows, n)), 0.0), axis=1, keepdims=True)
    full = jnp.broadcast_to(col, (rows, LANES))
    if rows > n:
        full = jnp.where(lax.broadcasted_iota(jnp.int32, (rows, LANES), 0) < n, full, 1.0)
    return full


def column_to_lane(col, n):
    part = col[:, :n]
    r = lax.broadcasted_iota(jnp.int32, part.shape, 0)
    c = lax.broadcasted_iota(jnp.int32, part.shape, 1)
    return jnp.sum(jnp.where(r == c, part, 0.0), axis=0, keepdims=True)


def total(x):
    return jnp.sum(jnp.sum(x, axis=0, keepdims=True), axis=1, keepdims=True)


def stats_kernel(n_dev, x_hbm, h_hbm, dyi_hbm, dyo_hbm, wi_hbm, wo_hbm, ri_hbm, ci_hbm, ro_hbm, co_hbm,
                 beta_s, rel_s, crms_s, cnorm_s,
                 di, do, wi, wo, rcol, acol, cnew, kout,
                 x_v, h_v, ring, tail, dyo_v, ri_v, ci_v, ro_v, co_v,
                 part, pair, recv, cden, bden, rsum, recv2,
                 in_sem, ring_sem, tail_sem, dyo_sem, w_sem,
                 pair_send, pair_recv, all_send, all_recv, two_send, two_recv):
    me = lax.axis_index('tp')
    core = lax.rem(me, 2)
    chip = me // 2
    partner = me + 1 - 2 * core
    nk, ni, nff = di.shape
    no, nd = wo.shape[0], wo.shape[1]
    n_super = nff // SUPER
    tail_cols = nff - n_super * SUPER
    rows_in, rows_out = ni * n_dev, no * n_dev
    no_pad = -(-no // 8) * 8

    barrier = pltpu.get_barrier_semaphore()
    for d in range(1, n_dev):
        pl.semaphore_signal(barrier, inc=1, device_id=(lax.rem(me + d, n_dev),), device_id_type=pl.DeviceIdType.MESH)

    small = [pltpu.make_async_copy(h_hbm, h_v, in_sem.at[0])]
    for a, b in ((ro_hbm, ro_v), (co_hbm, co_v), (ri_hbm, ri_v), (ci_hbm, ci_v), (x_hbm, x_v)):
        small.append(pltpu.make_async_copy(a, b, in_sem.at[len(small)]))
    n_out = nd // CHUNK
    dyo_cp = [pltpu.make_async_copy(dyo_hbm.at[:, pl.ds(c * CHUNK, CHUNK)], dyo_v.at[:, pl.ds(c * CHUNK, CHUNK)],
                                    dyo_sem.at[c]) for c in range(n_out)]
    def super_copy(k, c, slot):
        return pltpu.make_async_copy(dyi_hbm.at[k, pl.ds(c * SUPER, SUPER), :], ring.at[slot], ring_sem.at[slot])

    tail_cp = [pltpu.make_async_copy(dyi_hbm.at[k, pl.ds(n_super * SUPER, tail_cols), :], tail.at[k], tail_sem.at[k])
               for k in range(nk)]
    w_cp = [pltpu.make_async_copy(wi_hbm.at[k], wi.at[k], w_sem.at[k]) for k in range(nk)]
    w_cp.append(pltpu.make_async_copy(wo_hbm, wo, w_sem.at[nk]))

    small[0].start()
    for cp in dyo_cp:
        cp.start()
    for cp in small[1:]:
        cp.start()
    sequence = [(0, 0), (0, 1), (0, 2), (1, 2), (1, 0), (1, 1)]
    super_copy(*sequence[0], 0).start()
    super_copy(*sequence[1], 1).start()
    for cp in tail_cp:
        cp.start()

    part[...] = jnp.zeros_like(part)
    cden[...] = jnp.ones_like(cden)
    for cp in small[1:5]:
        cp.wait()
    for q in range(nd // LANES):
        cden[pl.ds(OUT_ROW + q, 1), :] = co_v[:, pl.ds(q * LANES, LANES)]
    for k in range(nk):
        for q in range(nff // LANES):
            cden[pl.ds(IN_ROW + IN_STEP * k + q, 1), :] = ci_v[pl.ds(k, 1), pl.ds(q * LANES, LANES)]
        rest = nff % LANES
        if rest:
            cden[pl.ds(IN_ROW + IN_STEP * k + nff // LANES, 1), pl.ds(0, rest)] = (
                ci_v[pl.ds(k, 1), pl.ds(nff - rest, rest)])
    for k in range(nk):
        vec = ri_v[pl.ds(k, 1), :]
        for p in range(0, ni, LANES):
            n = min(LANES, ni - p)
            rcol[pl.ds(k * ni + p, n), :] = lane_to_column(vec[:, p:p + n], n)
    vec = ro_v[...]
    for p in range(0, no, LANES):
        n = min(LANES, no - p)
        rows = -(-n // 8) * 8
        rcol[pl.ds(nk * ni + p, rows), :] = lane_to_column(vec[:, p:p + n], rows)
    lane = lax.broadcasted_iota(jnp.int32, (1, LANES), 1)
    row_sums = jnp.where(lane == 0, jnp.sum(ri_v[pl.ds(0, 1), :], axis=1, keepdims=True), 0.0)
    row_sums += jnp.where(lane == 1, jnp.sum(ri_v[pl.ds(1, 1), :], axis=1, keepdims=True), 0.0)
    row_sums += jnp.where(lane == 2, jnp.sum(vec, axis=1, keepdims=True), 0.0)
    part[pl.ds(SCALAR_ROW, 1), :] = row_sums

    def pair_copy(g):
        start, size = GROUPS[g]
        rows = pl.ds(pl.multiple_of(start + (1 - core) * (size // 2), 8), size // 2)
        return pltpu.make_async_remote_copy(src_ref=part.at[rows, :], dst_ref=pair.at[rows, :],
                                            send_sem=pair_send.at[g], recv_sem=pair_recv.at[g],
                                            device_id=(partner,), device_id_type=pl.DeviceIdType.MESH)

    def all_copy(g, d):
        start, size = GROUPS[g]
        rows = pl.ds(pl.multiple_of(start + core * (size // 2), 8), size // 2)
        dest = lax.rem(me + d, n_dev)
        return pltpu.make_async_remote_copy(src_ref=recv.at[chip, rows, :], dst_ref=recv.at[chip, rows, :],
                                            send_sem=all_send.at[g, d], recv_sem=all_recv.at[g, me],
                                            device_id=(dest,), device_id_type=pl.DeviceIdType.MESH)

    def all_wait(g, d):
        start, size = GROUPS[g]
        src = lax.rem(me + d, n_dev)
        rows = pl.ds(pl.multiple_of(start + lax.rem(src, 2) * (size // 2), 8), size // 2)
        ref = recv.at[src // 2, rows, :]
        pltpu.make_async_remote_copy(src_ref=ref, dst_ref=ref, send_sem=all_send.at[g, d], recv_sem=all_recv.at[g, src],
                                     device_id=(src,), device_id_type=pl.DeviceIdType.MESH).wait_recv()

    def spread(g):
        start, size = GROUPS[g]
        pair_copy(g).wait_recv()
        rows = pl.ds(pl.multiple_of(start + core * (size // 2), 8), size // 2)
        recv[chip, rows, :] = part[rows, :] + pair[rows, :]
        for d in range(1, n_dev):
            all_copy(g, d).start()

    rsum[...] = jnp.zeros_like(rsum)

    def square_sums(g, row0, stat0):
        m, n = g.shape
        sq = g * g
        cols = jnp.sum(sq, axis=0, keepdims=True)
        acc = rsum[pl.ds(row0, m), :]
        for b in range(0, n, LANES):
            w = min(LANES, n - b)
            if w == LANES:
                acc += sq[:, b:b + w]
                part[pl.ds(stat0 + b // LANES, 1), :] = cols[:, b:b + w]
            else:
                acc = acc + jnp.concatenate([sq[:, b:b + w], jnp.zeros((m, LANES - w), F32)], axis=1)
                part[pl.ds(stat0 + b // LANES, 1), pl.ds(0, w)] = cols[:, b:b + w]
        rsum[pl.ds(row0, m), :] = acc

    small[0].wait()
    for c in range(n_out):
        dyo_cp[c].wait()
        for p in range(0, CHUNK, 256):
            col = c * CHUNK + p
            g = jnp.dot(h_v[...], dyo_v[:, pl.ds(col, 256)], preferred_element_type=F32)
            do[:, pl.ds(col, 256)] = g
            square_sums(g, nk * ni, OUT_ROW + col // LANES)
    pl.semaphore_wait(barrier, n_dev - 1)
    pair_copy(0).start()

    small[5].wait()

    def nt(dy):
        return lax.dot_general(x_v[...], dy, (((1,), (1,)), ((), ())), preferred_element_type=F32)

    def super_step(k, c, slot):
        for p in range(0, SUPER, 256):
            col = pl.multiple_of(c * SUPER + p, 256)
            g = nt(ring[slot, pl.ds(p, 256), :])
            di[k, :, pl.ds(col, 256)] = g
            square_sums(g, k * ni, IN_ROW + IN_STEP * k + c * (SUPER // LANES) + p // LANES)

    def tail_step(k):
        for p in range(0, tail_cols, 256):
            n = min(256, tail_cols - p)
            col = n_super * SUPER + p
            g = nt(tail[k, pl.ds(p, n), :])
            di[k, :, pl.ds(col, n)] = g
            square_sums(g, k * ni, IN_ROW + IN_STEP * k + col // LANES)

    def step(i):
        slot = i % SLOTS
        super_copy(*sequence[i], slot).wait()
        super_step(*sequence[i], slot)
        if i + SLOTS < len(sequence):
            super_copy(*sequence[i + SLOTS], slot).start()

    step(0)
    step(1)
    pair_copy(1).start()
    spread(0)
    step(2)
    tail_cp[0].wait()
    tail_step(0)
    pair_copy(2).start()
    spread(1)
    step(3)
    tail_cp[1].wait()
    tail_step(1)
    pair_copy(3).start()
    spread(2)
    step(4)
    pair_copy(4).start()
    spread(3)
    for cp in w_cp:
        cp.start()
    step(5)
    pair_copy(5).start()
    spread(4)
    spread(5)

    rsum[...] = jnp.broadcast_to(jnp.sum(rsum[...], axis=1, keepdims=True), rsum.shape)

    def w_square_in(k):
        def body(q, acc):
            w = wi[k, :, pl.ds(pl.multiple_of(q * LANES, LANES), LANES)]
            return acc + w * w
        acc = lax.fori_loop(0, nff // LANES, body, jnp.zeros((ni, LANES), F32))
        rest = nff % LANES
        w = wi[k, :, pl.ds(nff - rest, rest)]
        return total(acc) + total(w * w)

    def w_square_out():
        m = no // 8 * 8
        acc = jnp.zeros((8, nd), F32)
        acc = lax.fori_loop(0, m // 8, lambda i, a: a + jnp.square(wo[pl.ds(pl.multiple_of(i * 8, 8), 8), :]), acc)
        w = wo[pl.ds(m, no - m), :]
        return total(acc) + total(w * w)

    w_sq = []
    for k in range(nk):
        w_cp[k].wait()
        w_sq.append(w_square_in(k))
    w_cp[nk].wait()
    w_sq.append(w_square_out())

    for g in range(len(GROUPS)):
        for d in range(1, n_dev):
            all_wait(g, d)

    beta = jnp.full((1, 1), beta_s[0], F32)
    mix = 1.0 - beta
    tot = recv[0]
    for c in range(1, n_dev // 2):
        tot = tot + recv[c]
    bden[...] = tot
    seg = [(IN_ROW + IN_STEP * k, IN_STEP, k * ni, ni, rows_in, nff) for k in range(nk)]
    seg.append((OUT_ROW, SCALAR_ROW, nk * ni, no_pad, rows_out, nd))
    sums = [total(bden[pl.ds(a, n), :]) for a, n, *_ in seg]
    norm_sq = sums[0] + sums[1] + sums[2]
    scale = jnp.minimum(1.0, jnp.full((1, 1), cnorm_s[0], F32) / jnp.sqrt(norm_sq))
    row_tot = bden[pl.ds(SCALAR_ROW, 1), :]
    for j, (a, n, ra, rn, m_all, n_all) in enumerate(seg):
        c2 = beta * cden[pl.ds(a, n), :] + mix * (scale * (scale * bden[pl.ds(a, n), :]) * (1.0 / m_all) + EPS_ONE)
        cnew[pl.ds(a, n), :] = c2
        bden[pl.ds(a, n), :] = lax.rsqrt(c2)
        r2 = beta * rcol[pl.ds(ra, rn), :] + mix * (scale * (scale * rsum[pl.ds(ra, rn), :]) * (1.0 / n_all) + EPS_ONE)
        rcol[pl.ds(ra, rn), :] = r2
        r_all = jnp.sum(jnp.where(lane == j, row_tot, 0.0), axis=1, keepdims=True)
        level = beta * (r_all / m_all) + mix * (scale * (scale * (sums[j] / n_all)) * (1.0 / m_all) + EPS_ONE)
        acol[pl.ds(ra, rn), :] = lax.rsqrt(r2 / level)

    def u_block(ref, k, row0, m, col, w, brow):
        s = jnp.broadcast_to(scale, (m, w))
        b = jnp.broadcast_to(bden[pl.ds(brow, 1), pl.ds(0, w)], (m, w))
        idx = (pl.ds(row0, m), pl.ds(col, w)) if k is None else (k, pl.ds(row0, m), pl.ds(col, w))
        t = (s * ref[idx]) * b
        ref[idx] = t
        return t * t

    u_sq = []
    for k in range(nk):
        def body(q, acc, k=k):
            return acc + u_block(di, k, 0, ni, pl.multiple_of(q * LANES, LANES), LANES, IN_ROW + IN_STEP * k + q)
        acc = lax.fori_loop(0, nff // LANES, body, jnp.zeros((ni, LANES), F32))
        a = acol[pl.ds(k * ni, ni), :]
        u = total(acc * a * a)
        rest = nff % LANES
        if rest:
            acc = u_block(di, k, 0, ni, nff - rest, rest, IN_ROW + IN_STEP * k + nff // LANES)
            a = acol[pl.ds(k * ni, ni), pl.ds(0, rest)]
            u = u + total(acc * a * a)
        u_sq.append(u)
    u = jnp.zeros((1, 1), F32)
    for row0, m in ((0, 144), (144, 144), (288, no - 288)):
        def body(q, acc, row0=row0, m=m):
            return acc + u_block(do, None, row0, m, pl.multiple_of(q * LANES, LANES), LANES, OUT_ROW + q)
        acc = lax.fori_loop(0, nd // LANES, body, jnp.zeros((m, LANES), F32))
        a = acol[pl.ds(nk * ni + row0, m), :]
        u = u + total(acc * a * a)
    u_sq.append(u)

    msg = jnp.zeros((1, LANES), F32)
    for j in range(3):
        msg = msg + jnp.where(lane == j, u_sq[j], 0.0) + jnp.where(lane == 3 + j, w_sq[j], 0.0)
    recv2[me] = msg

    def two_copy(d):
        dest = lax.rem(me + d, n_dev)
        return pltpu.make_async_remote_copy(src_ref=recv2.at[me], dst_ref=recv2.at[me], send_sem=two_send.at[d],
                                            recv_sem=two_recv.at[me], device_id=(dest,),
                                            device_id_type=pl.DeviceIdType.MESH)

    for d in range(1, n_dev):
        two_copy(d).start()
    for g in range(len(GROUPS)):
        pair_copy(g).wait_send()
        for d in range(1, n_dev):
            all_copy(g, d).wait_send()
    for d in range(1, n_dev):
        src = lax.rem(me + d, n_dev)
        ref = recv2.at[src]
        pltpu.make_async_remote_copy(src_ref=ref, dst_ref=ref, send_sem=two_send.at[d], recv_sem=two_recv.at[src],
                                     device_id=(src,), device_id_type=pl.DeviceIdType.MESH).wait_recv()
    all_sums = recv2[0]
    for c in range(1, n_dev):
        all_sums = all_sums + recv2[c]
    for j, (_, _, _, _, m_all, n_all) in enumerate(seg):
        u = jnp.sum(jnp.where(lane == j, all_sums, 0.0), axis=1, keepdims=True)
        w = jnp.sum(jnp.where(lane == 3 + j, all_sums, 0.0), axis=1, keepdims=True)
        u_rms = jnp.sqrt(u / (m_all * n_all))
        w_rms = jnp.sqrt(w / (m_all * n_all))
        step_size = jnp.full((1, 1), rel_s[0], F32) * jnp.maximum(EPS_TWO, w_rms)
        k = step_size / jnp.maximum(1.0, u_rms / jnp.full((1, 1), crms_s[0], F32))
        kout[pl.ds(j, 1), :] = jnp.broadcast_to(k, (1, LANES))
    for d in range(1, n_dev):
        two_copy(d).wait_send()


B_IN = 32


def update_kernel(di, do, wi, wo, rcol, acol, cnew, kout, wi_out, ri_out, ci_out, wo_out, ro_out, co_out,
                  buf_in, buf_out, sem_in, sem_out):
    nk, ni, nff = di.shape
    nd = do.shape[1]
    no = wo_out.shape[0]
    steps = ni // B_IN

    def in_copy(k, i, slot):
        return pltpu.make_async_copy(buf_in.at[slot], wi_out.at[k, pl.ds(i * B_IN, B_IN), :], sem_in.at[slot])

    def widths(n):
        return [(c, min(LANES, n - c)) for c in range(0, n, LANES)]

    pend = [None] * buf_in.shape[0]
    for k in range(nk):
        kk = jnp.broadcast_to(kout[pl.ds(k, 1), :], (B_IN, LANES))
        for i in range(steps):
            slot = (k * steps + i) % buf_in.shape[0]
            if pend[slot] is not None:
                pend[slot].wait()
            a = acol[pl.ds(k * ni + i * B_IN, B_IN), :]
            rows = pl.ds(i * B_IN, B_IN)

            def body(q, _, k=k, rows=rows, slot=slot, a=a, kk=kk):
                c = pl.ds(pl.multiple_of(q * LANES, LANES), LANES)
                buf_in[slot, :, c] = wi[k, rows, c] - kk * (di[k, rows, c] * a)
                return 0
            lax.fori_loop(0, nff // LANES, body, 0, unroll=4)
            rest = nff % LANES
            if rest:
                c = pl.ds(nff - rest, rest)
                buf_in[slot, :, c] = wi[k, rows, c] - kk[:, :rest] * (di[k, rows, c] * a[:, :rest])
            cp = in_copy(k, i, slot)
            cp.start()
            pend[slot] = cp
    pend_out = [None] * buf_out.shape[0]
    for i in range(nd // CHUNK):
        slot = i % buf_out.shape[0]
        if pend_out[slot] is not None:
            pend_out[slot].wait()
        kk = jnp.broadcast_to(kout[pl.ds(nk, 1), :], (8, LANES))

        def rows_of(o, n, i=i, slot=slot, kk=kk):
            r = pl.ds(o, n)
            a = acol[pl.ds(nk * ni + o, n), :]
            for c in range(0, CHUNK, LANES):
                cc = pl.ds(i * CHUNK + c, LANES)
                buf_out[slot, r, pl.ds(c, LANES)] = wo[r, cc] - kk[:n] * (do[r, cc] * a)

        def body(q, _, rows_of=rows_of):
            rows_of(pl.multiple_of(q * 8, 8), 8)
            return 0
        lax.fori_loop(0, no // 8, body, 0, unroll=4)
        if no % 8:
            rows_of(no // 8 * 8, no % 8)
        cols = pl.ds(i * CHUNK, CHUNK)
        cp = pltpu.make_async_copy(buf_out.at[slot], wo_out.at[:, cols], sem_out.at[slot])
        cp.start()
        pend_out[slot] = cp
    for q in range(nd // LANES):
        co_out[:, pl.ds(q * LANES, LANES)] = cnew[pl.ds(OUT_ROW + q, 1), :]
    for k in range(nk):
        for c, n in widths(nff):
            ci_out[pl.ds(k, 1), pl.ds(c, n)] = cnew[pl.ds(IN_ROW + IN_STEP * k + c // LANES, 1), pl.ds(0, n)]
        for c, n in widths(ni):
            ri_out[pl.ds(k, 1), pl.ds(c, n)] = column_to_lane(rcol[pl.ds(k * ni + c, n), :], n)
    for c, n in widths(no):
        ro_out[:, pl.ds(c, n)] = column_to_lane(rcol[pl.ds(nk * ni + c, -(-n // 8) * 8), :], n)
    for cp in pend + pend_out:
        if cp is not None:
            cp.wait()


def solution(mesh):
    n_dev = mesh.shape['tp']

    def local_step(x_norm, hid_act, dy_in, dy_out, w_in, w_out, row_in, col_in, row_out, col_out,
                   beta_two, rel_step, clip_rms, clip_norm):
        t, ni = x_norm.shape
        no = hid_act.shape[1]
        nk, _, nff = dy_in.shape
        nd = dy_out.shape[1]
        no_pad = -(-no // 8) * 8
        tail_cols = nff - nff // SUPER * SUPER
        vm = pl.BlockSpec(memory_space=pltpu.VMEM)
        hb = pl.BlockSpec(memory_space=pltpu.HBM)
        sm = pl.BlockSpec(memory_space=pltpu.SMEM)
        dma = pltpu.SemaphoreType.DMA
        n_rows = nk * ni + no_pad
        a_out = [pltpu.VMEM((nk, ni, nff), F32), pltpu.VMEM((no, nd), F32),
                 pltpu.VMEM((nk, ni, nff), F32), pltpu.VMEM((no, nd), F32),
                 pltpu.VMEM((n_rows, LANES), F32), pltpu.VMEM((n_rows, LANES), F32),
                 pltpu.VMEM((STAT_ROWS, LANES), F32), pltpu.VMEM((8, LANES), F32)]
        ng = len(GROUPS)
        outs = pl.pallas_call(
            lambda *refs: stats_kernel(n_dev, *refs),
            out_shape=a_out,
            in_specs=[hb] * 10 + [sm] * 4,
            out_specs=[vm] * len(a_out),
            scratch_shapes=[
                pltpu.VMEM((ni, t), BF16), pltpu.VMEM((no, t), BF16), pltpu.VMEM((SLOTS, SUPER, t), BF16),
                pltpu.VMEM((nk, tail_cols, t), BF16), pltpu.VMEM((t, nd), BF16),
                pltpu.VMEM((nk, ni), F32), pltpu.VMEM((nk, nff), F32), pltpu.VMEM((1, no), F32),
                pltpu.VMEM((1, nd), F32),
                pltpu.VMEM((STAT_ROWS, LANES), F32), pltpu.VMEM((STAT_ROWS, LANES), F32),
                pltpu.VMEM((n_dev // 2, STAT_ROWS, LANES), F32), pltpu.VMEM((STAT_ROWS, LANES), F32),
                pltpu.VMEM((STAT_ROWS, LANES), F32), pltpu.VMEM((n_rows, LANES), F32),
                pltpu.VMEM((n_dev, 1, LANES), F32),
                dma((6,)), dma((SLOTS,)), dma((nk,)), dma((nd // CHUNK,)), dma((nk + 1,)),
                dma((ng,)), dma((ng,)), dma((ng, n_dev)), dma((ng, n_dev)), dma((n_dev,)), dma((n_dev,)),
            ],
            compiler_params=pltpu.CompilerParams(collective_id=0, has_side_effects=True,
                                                 vmem_limit_bytes=30 * 1024 * 1024),
            name="stats",
        )(x_norm.T, hid_act.T, jnp.swapaxes(dy_in, 1, 2), dy_out, w_in, w_out, row_in, col_in,
          row_out.reshape(1, no), col_out.reshape(1, nd),
          beta_two.reshape(1), rel_step.reshape(1), clip_rms.reshape(1), clip_norm.reshape(1))
        outs = [pltpu.with_memory_space_constraint(o, pltpu.VMEM) for o in outs]
        b_out = [jax.ShapeDtypeStruct(w_in.shape, F32), jax.ShapeDtypeStruct(row_in.shape, F32),
                 jax.ShapeDtypeStruct(col_in.shape, F32), jax.ShapeDtypeStruct(w_out.shape, F32),
                 jax.ShapeDtypeStruct((1, no), F32), jax.ShapeDtypeStruct((1, nd), F32)]
        wi_new, ri_new, ci_new, wo_new, ro_new, co_new = pl.pallas_call(
            update_kernel,
            out_shape=b_out,
            in_specs=[vm] * len(outs),
            out_specs=[hb, vm, vm, hb, vm, vm],
            scratch_shapes=[pltpu.VMEM((4, B_IN, nff), F32), pltpu.VMEM((2, no, CHUNK), F32), dma((4,)), dma((2,))],
            compiler_params=pltpu.CompilerParams(vmem_limit_bytes=12 * 1024 * 1024),
            name="update",
        )(*outs)
        return (wi_new, ri_new, ci_new, wo_new, ro_new.reshape(no), co_new.reshape(nd))

    in_specs = (P(None, 'tp'), P(None, 'tp'), P(), P(), P(None, 'tp', None), P('tp', None),
                P(None, 'tp'), P(), P('tp'), P(), P(), P(), P(), P())
    out_specs = (P(None, 'tp', None), P(None, 'tp'), P(), P('tp', None), P('tp'), P())
    return jax.shard_map(local_step, mesh=mesh, in_specs=in_specs, out_specs=out_specs, check_vma=False)
```

```python
import jax
import jax.numpy as jnp
from jax import lax
from jax.experimental import pallas as pl
from jax.experimental.pallas import tpu as pltpu
from jax.sharding import PartitionSpec as P

MESH = pl.DeviceIdType.MESH
EPS_ONE = 1e-30
EPS_TWO = 1e-3
LANES = 128
F32 = jnp.float32
BF16 = jnp.bfloat16

OUT_ROW, IN_ROW, IN_STEP, STAT_ROWS = 0, 32, 64, 160
SCALAR_ROW = 24
STAGED = ((0, 32), (32, 64), (128, 32))
DIRECT_ROW = 96
DIRECT = ((112, 16), (96, 8), (104, 8))
CHUNK = 512
SUPER = 2048
HALF = 1024
SLOTS = 4
SCOPED = 30 * 1024 * 1024
PIECE = 256


def scope(name):
    pass


def lane_to_column(vec, rows):
    n = vec.shape[1]
    r = lax.broadcasted_iota(jnp.int32, (rows, n), 0)
    c = lax.broadcasted_iota(jnp.int32, (rows, n), 1)
    col = jnp.sum(jnp.where(r == c, jnp.broadcast_to(vec, (rows, n)), 0.0), axis=1, keepdims=True)
    full = jnp.broadcast_to(col, (rows, LANES))
    if rows > n:
        full = jnp.where(lax.broadcasted_iota(jnp.int32, (rows, LANES), 0) < n, full, 1.0)
    return full


def column_to_lane(col, n):
    part = col[:, :n]
    r = lax.broadcasted_iota(jnp.int32, part.shape, 0)
    c = lax.broadcasted_iota(jnp.int32, part.shape, 1)
    return jnp.sum(jnp.where(r == c, part, 0.0), axis=0, keepdims=True)


def total(x):
    return jnp.sum(jnp.sum(x, axis=0, keepdims=True), axis=1, keepdims=True)


def stats_kernel(n_dev, x_hbm, h_hbm, dyo_hbm, dyi_hbm, wi_hbm, wo_hbm, ri_hbm, ci_hbm, ro_hbm, co_hbm,
                 beta_s, rel_s, crms_s, cnorm_s,
                 di, do, wi, wo, rcol, acol, cnew, bden, kout,
                 x_v, h_v, dyo_v, ring, tail, ri_v, ci_v, ro_v, co_v, part, pair, tot, recv, recv_all, cden, rsum, recv2,
                 in_sem, dyo_sem, ring_sem, tail_sem, w_sem, pair_sem, chip_sem, back_sem, all_sem, two_sem):
    me = lax.axis_index('tp')
    core = lax.rem(me, 2)
    chip = me // 2
    partner = me + 1 - 2 * core
    nk, ni, nff = di.shape
    no, nd = wo.shape
    no_pad = -(-no // 8) * 8
    n_super = nff // SUPER
    tail_cols = nff - n_super * SUPER
    rows_in, rows_out = ni * n_dev, no * n_dev
    n_chip = n_dev // 2

    barrier = pltpu.get_barrier_semaphore()
    for d in range(1, n_dev):
        pl.semaphore_signal(barrier, inc=1, device_id=(lax.rem(me + d, n_dev),), device_id_type=MESH)

    scope("init")
    sequence = [(0, c) for c in range(n_super)] + [(1, c) for c in range(n_super - 1, -1, -1)]

    def half_copy(i, p):
        k, c = sequence[i]
        return pltpu.make_async_copy(dyi_hbm.at[k, pl.ds(c * SUPER + p * HALF, HALF), :],
                                     ring.at[i % SLOTS, pl.ds(p * HALF, HALF), :], ring_sem.at[i % SLOTS, p])

    def super_start(i):
        half_copy(i, 0).start()
        half_copy(i, 1).start()

    def super_wait(i):
        half_copy(i, 0).wait()
        half_copy(i, 1).wait()

    tail_cp = [pltpu.make_async_copy(dyi_hbm.at[k, pl.ds(n_super * SUPER, tail_cols), :], tail.at[k], tail_sem.at[k])
               for k in range(nk)]
    w_cp = [pltpu.make_async_copy(wi_hbm.at[k], wi.at[k], w_sem.at[k]) for k in range(nk)]
    w_cp.append(pltpu.make_async_copy(wo_hbm, wo, w_sem.at[nk]))
    small = [pltpu.make_async_copy(a, b, in_sem.at[i]) for i, (a, b) in enumerate(
        ((ro_hbm, ro_v), (ri_hbm, ri_v), (co_hbm, co_v), (ci_hbm, ci_v), (h_hbm, h_v), (x_hbm, x_v)))]
    dyo_cp = [pltpu.make_async_copy(dyo_hbm.at[:, pl.ds(c, CHUNK)], dyo_v.at[:, pl.ds(c, CHUNK)],
                                    dyo_sem.at[c // CHUNK]) for c in range(0, nd, CHUNK)]
    for cp in small[4:5] + dyo_cp[:2]:
        cp.start()
    part[...] = jnp.zeros_like(part)
    rsum[...] = jnp.zeros_like(rsum)

    def halves(start, size, c):
        return pl.ds(pl.multiple_of(start + c * (size // 2), 8), size // 2)

    def remote(src, dst, sem, device):
        return pltpu.make_async_remote_copy(src_ref=src, dst_ref=dst, send_sem=sem.at[0], recv_sem=sem.at[1],
                                            device_id=(device,), device_id_type=MESH)

    def pair_copy(g):
        rows = halves(*STAGED[g], 1 - core)
        return remote(part.at[rows, :], pair.at[rows, :], pair_sem.at[g], partner)

    def chip_copy(g, d):
        ref = recv.at[chip, halves(*STAGED[g], core), :]
        return remote(ref, ref, chip_sem.at[g], lax.rem(me + 2 * d, n_dev))

    def back_copy(g):
        ref = tot.at[halves(*STAGED[g], core), :]
        return remote(ref, ref, back_sem.at[g], partner)

    def all_copy(g, d):
        start, size = DIRECT[g]
        ref = recv_all.at[me, pl.ds(start - DIRECT_ROW, size), :]
        return remote(ref, ref, all_sem.at[g], lax.rem(me + d, n_dev))

    def two_copy(d):
        return remote(recv2.at[me], recv2.at[me], two_sem, lax.rem(me + d, n_dev))

    def bytes_of(ref, sem):
        pltpu.make_async_copy(ref, ref, sem).wait()

    def chip_stage(g):
        rows = halves(*STAGED[g], core)
        pair_copy(g).wait_recv()
        recv[chip, rows, :] = part[rows, :] + pair[rows, :]
        for d in range(1, n_chip):
            chip_copy(g, d).start()

    def back_stage(g):
        start, size = STAGED[g]
        rows = halves(start, size, core)
        bytes_of(recv.at[pl.ds(0, n_chip - 1), rows, :], chip_sem.at[g, 1])
        t = recv[0, rows, :]
        for c in range(1, n_chip):
            t = t + recv[c, rows, :]
        tot[rows, :] = t
        back_copy(g).start()

    def direct_stage(g):
        start, size = DIRECT[g]
        rows = pl.ds(start - DIRECT_ROW, size)
        recv_all[me, rows, :] = part[pl.ds(start, size), :]
        for d in range(1, n_dev):
            all_copy(g, d).start()

    def square_sums(g, row0, stat0):
        m, n = g.shape
        sq = g * g
        cols = jnp.sum(sq, axis=0, keepdims=True)
        acc = rsum[pl.ds(row0, m), :]
        for b in range(0, n, LANES):
            w = min(LANES, n - b)
            if w == LANES:
                acc += sq[:, b:b + w]
                part[pl.ds(stat0 + b // LANES, 1), :] = cols[:, b:b + w]
            else:
                acc = acc + jnp.concatenate([sq[:, b:b + w], jnp.zeros((m, LANES - w), F32)], axis=1)
                part[pl.ds(stat0 + b // LANES, 1), pl.ds(0, w)] = cols[:, b:b + w]
        rsum[pl.ds(row0, m), :] = acc

    def nt(dy):
        return lax.dot_general(dy, x_v[...], (((1,), (1,)), ((), ())), preferred_element_type=F32).T

    def in_piece(k, col, dy):
        g = nt(dy)
        di[k, :, pl.ds(col, g.shape[1])] = g
        square_sums(g, k * ni, IN_ROW + IN_STEP * k + col // LANES)

    def super_step(i, start=0, stop=SUPER):
        k, c = sequence[i]
        for p in range(start, stop, PIECE):
            in_piece(k, c * SUPER + p, ring[i % SLOTS, pl.ds(p, PIECE), :])

    def tail_step(k):
        for p in range(0, tail_cols, 256):
            in_piece(k, n_super * SUPER + p, tail[k, pl.ds(p, min(256, tail_cols - p)), :])

    def out_piece(start, stop):
        for col in range(start, stop, 256):
            g = jnp.dot(h_v[...], dyo_v[:, pl.ds(col, 256)], preferred_element_type=F32)
            do[:, pl.ds(col, 256)] = g
            square_sums(g, nk * ni, OUT_ROW + col // LANES)

    scope("out")
    small[4].wait()
    dyo_cp[0].wait()
    for cp in dyo_cp[2:4]:
        cp.start()
    out_piece(0, CHUNK)
    dyo_cp[1].wait()
    for cp in dyo_cp[4:] + small[5:6] + small[:4]:
        cp.start()
    half_copy(0, 0).start()
    scope("out1")
    dyo_cp[2].wait()
    out_piece(CHUNK, 3 * CHUNK)
    half_copy(0, 1).start()
    super_start(1)
    scope("out2")
    for cp in dyo_cp[3:]:
        cp.wait()
    out_piece(3 * CHUNK, nd)
    for cp in small[:2]:
        cp.wait()
    lane = lax.broadcasted_iota(jnp.int32, (1, LANES), 1)
    row_sums = jnp.where(lane == 2, jnp.sum(ro_v[...], axis=1, keepdims=True), 0.0)
    for k in range(nk):
        row_sums += jnp.where(lane == k, jnp.sum(ri_v[pl.ds(k, 1), :], axis=1, keepdims=True), 0.0)
    part[pl.ds(SCALAR_ROW, 1), :] = row_sums
    pl.semaphore_wait(barrier, n_dev - 1)
    pair_copy(0).start()

    scope("in0")
    small[5].wait()
    super_wait(0)
    super_start(2)
    tail_cp[0].start()
    super_step(0)
    chip_stage(0)
    scope("in1")
    super_wait(1)
    super_start(3)
    tail_cp[1].start()
    super_step(1)
    scope("in2")
    super_wait(2)
    tail_cp[0].wait()
    super_start(4)
    super_step(2)
    tail_step(0)
    pair_copy(1).start()
    scope("in3")
    super_wait(3)
    tail_cp[1].wait()
    super_start(5)
    super_step(3)
    tail_step(1)
    pair_copy(2).start()
    chip_stage(1)
    scope("in4")
    super_wait(4)
    super_step(4)
    direct_stage(0)
    chip_stage(2)
    scope("in5")
    super_wait(5)
    for cp in w_cp:
        cp.start()
    super_step(5, 0, HALF)
    direct_stage(1)
    super_step(5, HALF, SUPER)
    direct_stage(2)
    back_stage(0)

    scope("forms")
    for cp in small[2:4]:
        cp.wait()
    cden[...] = jnp.ones_like(cden)
    cden[pl.ds(OUT_ROW, nd // LANES), :] = co_v[...]
    for k in range(nk):
        for q in range(nff // LANES):
            cden[pl.ds(IN_ROW + IN_STEP * k + q, 1), :] = ci_v[pl.ds(k, 1), pl.ds(q * LANES, LANES)]
        rest = nff % LANES
        if rest:
            cden[pl.ds(IN_ROW + IN_STEP * k + nff // LANES, 1), pl.ds(0, rest)] = (
                ci_v[pl.ds(k, 1), pl.ds(nff - rest, rest)])
    for k in range(nk):
        vec = ri_v[pl.ds(k, 1), :]
        for p in range(0, ni, LANES):
            n = min(LANES, ni - p)
            rcol[pl.ds(k * ni + p, n), :] = lane_to_column(vec[:, p:p + n], n)
    vec = ro_v[...]
    for p in range(0, no, LANES):
        n = min(LANES, no - p)
        rows = -(-n // 8) * 8
        rcol[pl.ds(nk * ni + p, rows), :] = lane_to_column(vec[:, p:p + n], rows)
    rsum[...] = jnp.broadcast_to(jnp.sum(rsum[...], axis=1, keepdims=True), rsum.shape)
    back_stage(1)

    def w_square_in(k):
        def body(q, acc):
            w = wi[k, :, pl.ds(pl.multiple_of(q * LANES, LANES), LANES)]
            return acc + w * w
        acc = lax.fori_loop(0, nff // LANES, body, jnp.zeros((ni, LANES), F32), unroll=4)
        rest = nff % LANES
        w = wi[k, :, pl.ds(nff - rest, rest)]
        return total(acc) + total(w * w)

    def w_square_out():
        m = no // 8 * 8
        acc = jnp.zeros((8, nd), F32)
        acc = lax.fori_loop(0, m // 8, lambda i, a: a + jnp.square(wo[pl.ds(pl.multiple_of(i * 8, 8), 8), :]), acc,
                            unroll=4)
        w = wo[pl.ds(m, no - m), :]
        return total(acc) + total(w * w)

    scope("wsq")
    w_sq = []
    for k in range(nk):
        w_cp[k].wait()
        w_sq.append(w_square_in(k))
    scope("back2")
    back_stage(2)
    scope("wsq2")
    w_cp[nk].wait()
    w_sq.append(w_square_out())

    scope("wait1")
    for g in range(len(STAGED)):
        ref = tot.at[halves(*STAGED[g], 1 - core), :]
        bytes_of(ref, back_sem.at[g, 1])
    for g in range(len(DIRECT)):
        start, size = DIRECT[g]
        rows = pl.ds(start - DIRECT_ROW, size)
        bytes_of(recv_all.at[pl.ds(0, n_dev - 1), rows, :], all_sem.at[g, 1])
    t = recv_all[0]
    for c in range(1, n_dev):
        t = t + recv_all[c]
    tot[pl.ds(DIRECT_ROW, t.shape[0]), :] = t

    scope("stats")
    beta = jnp.full((1, 1), beta_s[()], F32)
    mix = 1.0 - beta
    seg = [(IN_ROW + IN_STEP * k, IN_STEP, k * ni, ni, rows_in, nff) for k in range(nk)]
    seg.append((OUT_ROW, SCALAR_ROW, nk * ni, no_pad, rows_out, nd))
    sums = [total(tot[pl.ds(a, n), :]) for a, n, *_ in seg]
    norm_sq = sums[0] + sums[1] + sums[2]
    scale = jnp.minimum(1.0, jnp.full((1, 1), cnorm_s[()], F32) / jnp.sqrt(norm_sq))
    row_tot = tot[pl.ds(SCALAR_ROW, 1), :]
    for j, (a, n, ra, rn, m_all, n_all) in enumerate(seg):
        c2 = beta * cden[pl.ds(a, n), :] + mix * (scale * (scale * tot[pl.ds(a, n), :]) * (1.0 / m_all) + EPS_ONE)
        cnew[pl.ds(a, n), :] = c2
        bden[pl.ds(a, n), :] = scale * lax.rsqrt(c2)
        r2 = beta * rcol[pl.ds(ra, rn), :] + mix * (scale * (scale * rsum[pl.ds(ra, rn), :]) * (1.0 / n_all) + EPS_ONE)
        rcol[pl.ds(ra, rn), :] = r2
        r_all = jnp.sum(jnp.where(lane == j, row_tot, 0.0), axis=1, keepdims=True)
        level = beta * (r_all / m_all) + mix * (scale * (scale * (sums[j] / n_all)) * (1.0 / m_all) + EPS_ONE)
        acol[pl.ds(ra, rn), :] = lax.rsqrt(r2 / level)

    def u_square(ref, k, row0, m, cols, stat0, arow):
        rows = pl.ds(row0, m)

        def block(col, w, brow):
            idx = (rows, pl.ds(col, w)) if k is None else (k, rows, pl.ds(col, w))
            t = ref[idx] * jnp.broadcast_to(bden[pl.ds(brow, 1), pl.ds(0, w)], (m, w))
            return t * t

        def body(i, acc):
            for q in range(4):
                col = pl.multiple_of(i * 4 * LANES + q * LANES, LANES)
                acc = acc + block(col, LANES, stat0 + i * 4 + q)
            return acc
        acc = lax.fori_loop(0, cols // LANES // 4, body, jnp.zeros((m, LANES), F32))
        a = acol[pl.ds(arow, m), :]
        u = total(acc * a * a)
        rest = cols % LANES
        if rest:
            a = acol[pl.ds(arow, m), pl.ds(0, rest)]
            u = u + total(block(cols - rest, rest, stat0 + cols // LANES) * a * a)
        return u

    scope("upass")
    u_sq = [u_square(di, k, 0, ni, nff, IN_ROW + IN_STEP * k, k * ni) for k in range(nk)]
    u_sq.append(sum(u_square(do, None, row0, m, nd, OUT_ROW, nk * ni + row0)
                    for row0, m in ((0, 144), (144, 144), (288, no - 288))))

    scope("x2")
    msg = jnp.zeros((1, LANES), F32)
    for j in range(3):
        msg = msg + jnp.where(lane == j, u_sq[j], 0.0) + jnp.where(lane == 3 + j, w_sq[j], 0.0)
    recv2[me] = msg
    for d in range(1, n_dev):
        two_copy(d).start()
    for g in range(len(STAGED)):
        pair_copy(g).wait_send()
        back_copy(g).wait_send()
        bytes_of(recv.at[pl.ds(0, n_chip - 1), halves(*STAGED[g], core), :], chip_sem.at[g, 0])
    for g in range(len(DIRECT)):
        start, size = DIRECT[g]
        bytes_of(recv_all.at[pl.ds(0, n_dev - 1), pl.ds(start - DIRECT_ROW, size), :], all_sem.at[g, 0])
    bytes_of(recv2.at[pl.ds(0, n_dev - 1)], two_sem.at[1])
    scope("fin")
    all_sums = recv2[0]
    for c in range(1, n_dev):
        all_sums = all_sums + recv2[c]
    for j, (_, _, _, _, m_all, n_all) in enumerate(seg):
        u = jnp.sum(jnp.where(lane == j, all_sums, 0.0), axis=1, keepdims=True)
        w = jnp.sum(jnp.where(lane == 3 + j, all_sums, 0.0), axis=1, keepdims=True)
        u_rms = jnp.sqrt(u / (m_all * n_all))
        w_rms = jnp.sqrt(w / (m_all * n_all))
        step_size = jnp.full((1, 1), rel_s[()], F32) * jnp.maximum(EPS_TWO, w_rms)
        k = step_size / jnp.maximum(1.0, u_rms / jnp.full((1, 1), crms_s[()], F32))
        kout[pl.ds(j, 1), :] = jnp.broadcast_to(k, (1, LANES))
    bytes_of(recv2.at[pl.ds(0, n_dev - 1)], two_sem.at[0])
    scope(None)


B_IN = 32


def update_kernel(di, do, wi, wo, rcol, acol, cnew, bden, kout, wi_out, ri_out, ci_out, wo_out, ro_out, co_out,
                  buf_in, buf_out, sem_in, sem_out):
    nk, ni, nff = di.shape
    no, nd = do.shape
    steps = ni // B_IN

    def in_copy(k, i, slot):
        return pltpu.make_async_copy(buf_in.at[slot], wi_out.at[k, pl.ds(i * B_IN, B_IN), :], sem_in.at[slot])

    def widths(n):
        return [(c, min(LANES, n - c)) for c in range(0, n, LANES)]

    def step_of(w, g, b, a, kk):
        return w - kk * ((g * jnp.broadcast_to(b, g.shape)) * a)

    pend = [None] * buf_in.shape[0]
    for k in range(nk):
        kk = jnp.broadcast_to(kout[pl.ds(k, 1), :], (B_IN, LANES))
        for i in range(steps):
            slot = (k * steps + i) % buf_in.shape[0]
            if pend[slot] is not None:
                pend[slot].wait()
            a = acol[pl.ds(k * ni + i * B_IN, B_IN), :]
            rows = pl.ds(i * B_IN, B_IN)
            for q, (c, n) in enumerate(widths(nff)):
                cc = pl.ds(c, n)
                b = bden[pl.ds(IN_ROW + IN_STEP * k + q, 1), pl.ds(0, n)]
                buf_in[slot, :, cc] = step_of(wi[k, rows, cc], di[k, rows, cc], b, a[:, :n], kk[:, :n])
            cp = in_copy(k, i, slot)
            cp.start()
            pend[slot] = cp
    pend_out = [None] * buf_out.shape[0]
    for i in range(nd // CHUNK):
        slot = i % buf_out.shape[0]
        if pend_out[slot] is not None:
            pend_out[slot].wait()
        kk = jnp.broadcast_to(kout[pl.ds(nk, 1), :], (40, LANES))
        bs = [bden[pl.ds(OUT_ROW + i * (CHUNK // LANES) + q, 1), :] for q in range(CHUNK // LANES)]

        def rows_of(o, n, i=i, slot=slot, kk=kk, bs=bs):
            r = pl.ds(o, n)
            a = acol[pl.ds(nk * ni + o, n), :]
            for q, b in enumerate(bs):
                cc = pl.ds(i * CHUNK + q * LANES, LANES)
                buf_out[slot, r, pl.ds(q * LANES, LANES)] = step_of(wo[r, cc], do[r, cc], b, a, kk[:n])

        for o in range(0, no, 40):
            rows_of(o, min(40, no - o))
        cp = pltpu.make_async_copy(buf_out.at[slot], wo_out.at[:, pl.ds(i * CHUNK, CHUNK)], sem_out.at[slot])
        cp.start()
        pend_out[slot] = cp
    co_out[...] = cnew[pl.ds(OUT_ROW, nd // LANES), :]
    for k in range(nk):
        for c, n in widths(nff):
            ci_out[pl.ds(k, 1), pl.ds(c, n)] = cnew[pl.ds(IN_ROW + IN_STEP * k + c // LANES, 1), pl.ds(0, n)]
        for c, n in widths(ni):
            ri_out[pl.ds(k, 1), pl.ds(c, n)] = column_to_lane(rcol[pl.ds(k * ni + c, n), :], n)
    for c, n in widths(no):
        ro_out[:, pl.ds(c, n)] = column_to_lane(rcol[pl.ds(nk * ni + c, -(-n // 8) * 8), :], n)
    for cp in pend + pend_out:
        if cp is not None:
            cp.wait()


def solution(mesh):
    n_dev = mesh.shape['tp']

    def local_step(x_norm, hid_act, dy_in, dy_out, w_in, w_out, row_in, col_in, row_out, col_out,
                   beta_two, rel_step, clip_rms, clip_norm):
        t, ni = x_norm.shape
        no = hid_act.shape[1]
        nk, _, nff = dy_in.shape
        nd = dy_out.shape[1]
        no_pad = -(-no // 8) * 8
        tail_cols = nff - nff // SUPER * SUPER
        vm = pl.BlockSpec(memory_space=pltpu.VMEM)
        hb = pl.BlockSpec(memory_space=pltpu.HBM)
        sm = pl.BlockSpec(memory_space=pltpu.SMEM)
        dma = pltpu.SemaphoreType.DMA
        n_rows = nk * ni + no_pad
        a_out = [pltpu.VMEM((nk, ni, nff), F32), pltpu.VMEM((no, nd), F32),
                 pltpu.VMEM((nk, ni, nff), F32), pltpu.VMEM((no, nd), F32),
                 pltpu.VMEM((n_rows, LANES), F32), pltpu.VMEM((n_rows, LANES), F32),
                 pltpu.VMEM((STAT_ROWS, LANES), F32), pltpu.VMEM((STAT_ROWS, LANES), F32),
                 pltpu.VMEM((8, LANES), F32)]
        ns, ng = len(STAGED), len(DIRECT)
        stat = pltpu.VMEM((STAT_ROWS, LANES), F32)
        outs = pl.pallas_call(
            lambda *refs: stats_kernel(n_dev, *refs),
            out_shape=a_out,
            in_specs=[hb] * 10 + [sm] * 4,
            out_specs=[vm] * len(a_out),
            scratch_shapes=[
                pltpu.VMEM((ni, t), BF16), pltpu.VMEM((no, t), BF16), pltpu.VMEM((t, nd), BF16),
                pltpu.VMEM((SLOTS, SUPER, t), BF16), pltpu.VMEM((nk, tail_cols, t), BF16),
                pltpu.VMEM((nk, ni), F32), pltpu.VMEM((nk, nff), F32), pltpu.VMEM((1, no), F32),
                pltpu.VMEM((nd // LANES, LANES), F32),
                stat, stat, stat, pltpu.VMEM((n_dev // 2, STAT_ROWS, LANES), F32),
                pltpu.VMEM((n_dev, sum(n for _, n in DIRECT), LANES), F32), stat,
                pltpu.VMEM((n_rows, LANES), F32), pltpu.VMEM((n_dev, 1, LANES), F32),
                dma((6,)), dma((nd // CHUNK,)), dma((SLOTS, 2)), dma((nk,)), dma((nk + 1,)),
                dma((ns, 2)), dma((ns, 2)), dma((ns, 2)), dma((ng, 2)), dma((2,)),
            ],
            compiler_params=pltpu.CompilerParams(collective_id=0, has_side_effects=True,
                                                 vmem_limit_bytes=SCOPED),
            name="stats",
        )(x_norm.T, hid_act.T, dy_out, jnp.swapaxes(dy_in, 1, 2), w_in, w_out, row_in, col_in,
          row_out.reshape(1, no), col_out.reshape(nd // LANES, LANES),
          beta_two, rel_step, clip_rms, clip_norm)
        outs = [pltpu.with_memory_space_constraint(o, pltpu.VMEM) for o in outs]
        b_out = [jax.ShapeDtypeStruct(w_in.shape, F32), jax.ShapeDtypeStruct(row_in.shape, F32),
                 jax.ShapeDtypeStruct(col_in.shape, F32), jax.ShapeDtypeStruct(w_out.shape, F32),
                 jax.ShapeDtypeStruct((1, no), F32), jax.ShapeDtypeStruct((nd // LANES, LANES), F32)]
        wi_new, ri_new, ci_new, wo_new, ro_new, co_new = pl.pallas_call(
            update_kernel,
            out_shape=b_out,
            in_specs=[vm] * len(outs),
            out_specs=[hb, vm, vm, hb, vm, vm],
            scratch_shapes=[pltpu.VMEM((4, B_IN, nff), F32), pltpu.VMEM((2, no, CHUNK), F32), dma((4,)), dma((2,))],
            compiler_params=pltpu.CompilerParams(vmem_limit_bytes=SCOPED),
            name="update",
        )(*outs)
        return (wi_new, ri_new, ci_new, wo_new, ro_new.reshape(no), co_new.reshape(nd))

    in_specs = (P(None, 'tp'), P(None, 'tp'), P(), P(), P(None, 'tp', None), P('tp', None),
                P(None, 'tp'), P(), P('tp'), P(), P(), P(), P(), P())
    out_specs = (P(None, 'tp', None), P(None, 'tp'), P(), P('tp', None), P('tp'), P())
    return jax.shard_map(local_step, mesh=mesh, in_specs=in_specs, out_specs=out_specs, check_vma=False)
```

```python
import jax
import jax.numpy as jnp
from jax import lax
from jax.experimental import pallas as pl
from jax.experimental.pallas import tpu as pltpu
from jax.sharding import PartitionSpec as P

MESH = pl.DeviceIdType.MESH
EPS_ONE = 1e-30
EPS_TWO = 1e-3
LANES = 128
F32 = jnp.float32
BF16 = jnp.bfloat16

OUT_ROW, IN_ROW, IN_STEP, STAT_ROWS = 0, 32, 64, 160
SCALAR_ROW = 24
STAGED = ((0, 32), (32, 64), (128, 32), (112, 16))
DIRECT_ROW = 96
DIRECT = ((96, 8), (104, 8))
CHUNK = 512
SUPER = 2048
HALF = 1024
SLOTS = 4
SCOPED = 30 * 1024 * 1024
PIECE = 256


def scope(name):
    pass


def lane_to_column(vec, rows):
    n = vec.shape[1]
    r = lax.broadcasted_iota(jnp.int32, (rows, n), 0)
    c = lax.broadcasted_iota(jnp.int32, (rows, n), 1)
    col = jnp.sum(jnp.where(r == c, jnp.broadcast_to(vec, (rows, n)), 0.0), axis=1, keepdims=True)
    full = jnp.broadcast_to(col, (rows, LANES))
    if rows > n:
        full = jnp.where(lax.broadcasted_iota(jnp.int32, (rows, LANES), 0) < n, full, 1.0)
    return full


def column_to_lane(col, n):
    part = col[:, :n]
    r = lax.broadcasted_iota(jnp.int32, part.shape, 0)
    c = lax.broadcasted_iota(jnp.int32, part.shape, 1)
    return jnp.sum(jnp.where(r == c, part, 0.0), axis=0, keepdims=True)


def total(x):
    return jnp.sum(jnp.sum(x, axis=0, keepdims=True), axis=1, keepdims=True)


def stats_kernel(n_dev, x_hbm, h_hbm, dyo_hbm, dyi_hbm, wi_hbm, wo_hbm, ri_hbm, ci_hbm, ro_hbm, co_hbm,
                 beta_s, rel_s, crms_s, cnorm_s,
                 di, do, wi, wo, rcol, acol, cnew, bden, kout,
                 x_v, h_v, dyo_v, ring, tail, raw, ri_v, ci_v, ro_v, co_v, part, pair, tot, recv, recv_all, cden, rsum, recv2,
                 in_sem, dyo_sem, ring_sem, tail_sem, w_sem, pair_sem, chip_sem, back_sem, all_sem, two_sem):
    me = lax.axis_index('tp')
    core = lax.rem(me, 2)
    chip = me // 2
    partner = me + 1 - 2 * core
    nk, ni, nff = di.shape
    no, nd = wo.shape
    no_pad = -(-no // 8) * 8
    n_super = nff // SUPER
    tail_cols = nff - n_super * SUPER
    rows_in, rows_out = ni * n_dev, no * n_dev
    n_chip = n_dev // 2

    barrier = pltpu.get_barrier_semaphore()
    for d in range(1, n_dev):
        pl.semaphore_signal(barrier, inc=1, device_id=(lax.rem(me + d, n_dev),), device_id_type=MESH)

    scope("init")
    sequence = [(0, c) for c in range(n_super)] + [(1, c) for c in range(n_super - 1, -1, -1)]

    def half_copy(i, p):
        k, c = sequence[i]
        return pltpu.make_async_copy(dyi_hbm.at[k, pl.ds(c * SUPER + p * HALF, HALF), :],
                                     ring.at[i % SLOTS, pl.ds(p * HALF, HALF), :], ring_sem.at[i % SLOTS, p])

    def super_start(i):
        half_copy(i, 0).start()
        half_copy(i, 1).start()

    def super_wait(i):
        half_copy(i, 0).wait()
        half_copy(i, 1).wait()

    tail_cp = [pltpu.make_async_copy(dyi_hbm.at[k, pl.ds(n_super * SUPER, tail_cols), :], tail.at[k], tail_sem.at[k])
               for k in range(nk)]
    w_cp = [pltpu.make_async_copy(wi_hbm.at[k], wi.at[k], w_sem.at[k]) for k in range(nk)]
    w_cp.append(pltpu.make_async_copy(wo_hbm, wo, w_sem.at[nk]))
    small = [pltpu.make_async_copy(a, b, in_sem.at[i]) for i, (a, b) in enumerate(
        ((ro_hbm, ro_v), (ri_hbm, ri_v), (co_hbm, co_v), (ci_hbm, ci_v), (h_hbm, h_v), (x_hbm, x_v)))]
    dyo_cp = [pltpu.make_async_copy(dyo_hbm.at[:, pl.ds(c, CHUNK)], dyo_v.at[:, pl.ds(c, CHUNK)],
                                    dyo_sem.at[c // CHUNK]) for c in range(0, nd, CHUNK)]
    for cp in small[4:5] + dyo_cp[:2]:
        cp.start()
    part[...] = jnp.zeros_like(part)
    rsum[...] = jnp.zeros_like(rsum)

    def halves(start, size, c):
        return pl.ds(pl.multiple_of(start + c * (size // 2), 8), size // 2)

    def remote(src, dst, sem, device):
        return pltpu.make_async_remote_copy(src_ref=src, dst_ref=dst, send_sem=sem.at[0], recv_sem=sem.at[1],
                                            device_id=(device,), device_id_type=MESH)

    def pair_copy(g):
        rows = halves(*STAGED[g], 1 - core)
        return remote(part.at[rows, :], pair.at[rows, :], pair_sem.at[g], partner)

    def chip_copy(g, d):
        ref = recv.at[chip, halves(*STAGED[g], core), :]
        return remote(ref, ref, chip_sem.at[g], lax.rem(me + 2 * d, n_dev))

    def back_copy(g):
        ref = tot.at[halves(*STAGED[g], core), :]
        return remote(ref, ref, back_sem.at[g], partner)

    def all_copy(g, d):
        start, size = DIRECT[g]
        ref = recv_all.at[me, pl.ds(start - DIRECT_ROW, size), :]
        return remote(ref, ref, all_sem.at[g], lax.rem(me + d, n_dev))

    def two_copy(d):
        return remote(recv2.at[me], recv2.at[me], two_sem, lax.rem(me + d, n_dev))

    def bytes_of(ref, sem):
        pltpu.make_async_copy(ref, ref, sem).wait()

    def chip_stage(g):
        rows = halves(*STAGED[g], core)
        pair_copy(g).wait_recv()
        recv[chip, rows, :] = part[rows, :] + pair[rows, :]
        for d in range(1, n_chip):
            chip_copy(g, d).start()

    def back_stage(g):
        start, size = STAGED[g]
        rows = halves(start, size, core)
        bytes_of(recv.at[pl.ds(0, n_chip - 1), rows, :], chip_sem.at[g, 1])
        t = recv[0, rows, :]
        for c in range(1, n_chip):
            t = t + recv[c, rows, :]
        tot[rows, :] = t
        back_copy(g).start()

    def direct_stage(g):
        start, size = DIRECT[g]
        rows = pl.ds(start - DIRECT_ROW, size)
        recv_all[me, rows, :] = part[pl.ds(start, size), :]
        for d in range(1, n_dev):
            all_copy(g, d).start()

    def square_sums(g, row0, stat0):
        m, n = g.shape
        sq = g * g
        cols = jnp.sum(sq, axis=0, keepdims=True)
        acc = rsum[pl.ds(row0, m), :]
        for b in range(0, n, LANES):
            w = min(LANES, n - b)
            if w == LANES:
                acc += sq[:, b:b + w]
                part[pl.ds(stat0 + b // LANES, 1), :] = cols[:, b:b + w]
            else:
                acc = acc + jnp.concatenate([sq[:, b:b + w], jnp.zeros((m, LANES - w), F32)], axis=1)
                part[pl.ds(stat0 + b // LANES, 1), pl.ds(0, w)] = cols[:, b:b + w]
        rsum[pl.ds(row0, m), :] = acc

    deferred = []

    def flush():
        for f in deferred:
            f()
        deferred.clear()

    def finish_in(k, col, g):
        g = g.T
        di[k, :, pl.ds(col, g.shape[1])] = g
        square_sums(g, k * ni, IN_ROW + IN_STEP * k + col // LANES)

    def finish_out(col):
        square_sums(do[:, pl.ds(col, 256)], nk * ni, OUT_ROW + col // LANES)

    def in_block(pieces, defer):
        for j, (k, col, n, ref) in enumerate(pieces):
            g = lax.dot_general(ref[...], x_v[...], (((1,), (1,)), ((), ())), preferred_element_type=F32)
            slot = j - len(pieces) + 2
            if defer and slot >= 0:
                raw[slot, pl.ds(0, n), :] = g
                deferred.append(lambda k=k, col=col, n=n, slot=slot: finish_in(k, col, raw[slot, pl.ds(0, n), :]))
            else:
                finish_in(k, col, g)

    def super_pieces(i, start=0, stop=SUPER):
        k, c = sequence[i]
        return [(k, c * SUPER + p, 256, ring.at[i % SLOTS, pl.ds(p, 256), :]) for p in range(start, stop, 256)]

    def tail_pieces(k):
        return [(k, n_super * SUPER + p, min(256, tail_cols - p), tail.at[k, pl.ds(p, min(256, tail_cols - p)), :])
                for p in range(0, tail_cols, 256)]

    def out_piece(start, stop):
        for col in range(start, stop, 256):
            do[:, pl.ds(col, 256)] = jnp.dot(h_v[...], dyo_v[:, pl.ds(col, 256)], preferred_element_type=F32)
            if col + 512 >= stop:
                deferred.append(lambda col=col: finish_out(col))
            else:
                finish_out(col)

    scope("out")
    small[4].wait()
    dyo_cp[0].wait()
    for cp in dyo_cp[2:4]:
        cp.start()
    out_piece(0, CHUNK)
    dyo_cp[1].wait()
    for cp in dyo_cp[4:] + small[5:6] + small[:4]:
        cp.start()
    half_copy(0, 0).start()
    scope("out1")
    dyo_cp[2].wait()
    flush()
    out_piece(CHUNK, 3 * CHUNK)
    half_copy(0, 1).start()
    super_start(1)
    scope("out2")
    for cp in dyo_cp[3:]:
        cp.wait()
    flush()
    out_piece(3 * CHUNK, nd)
    for cp in small[:2]:
        cp.wait()
    lane = lax.broadcasted_iota(jnp.int32, (1, LANES), 1)
    row_sums = jnp.where(lane == 2, jnp.sum(ro_v[...], axis=1, keepdims=True), 0.0)
    for k in range(nk):
        row_sums += jnp.where(lane == k, jnp.sum(ri_v[pl.ds(k, 1), :], axis=1, keepdims=True), 0.0)
    part[pl.ds(SCALAR_ROW, 1), :] = row_sums
    scope("in0")
    small[5].wait()
    super_wait(0)
    super_start(2)
    tail_cp[0].start()
    flush()
    in_block(super_pieces(0), True)
    pl.semaphore_wait(barrier, n_dev - 1)
    pair_copy(0).start()
    scope("in1")
    super_wait(1)
    super_start(3)
    tail_cp[1].start()
    flush()
    in_block(super_pieces(1), True)
    chip_stage(0)
    scope("in2")
    super_wait(2)
    tail_cp[0].wait()
    super_start(4)
    flush()
    in_block(super_pieces(2) + tail_pieces(0), False)
    pair_copy(1).start()
    scope("in3")
    super_wait(3)
    tail_cp[1].wait()
    super_start(5)
    in_block(super_pieces(3) + tail_pieces(1), False)
    pair_copy(2).start()
    chip_stage(1)
    scope("in4")
    super_wait(4)
    w_cp[0].start()
    in_block(super_pieces(4), False)
    pair_copy(3).start()
    chip_stage(2)
    scope("in5")
    super_wait(5)
    for cp in w_cp[1:]:
        cp.start()
    in_block(super_pieces(5, 0, HALF), False)
    direct_stage(0)
    chip_stage(3)
    in_block(super_pieces(5, HALF, SUPER), False)
    direct_stage(1)
    back_stage(0)

    scope("forms")
    for cp in small[2:4]:
        cp.wait()
    cden[...] = jnp.ones_like(cden)
    cden[pl.ds(OUT_ROW, nd // LANES), :] = co_v[...]
    for k in range(nk):
        for q in range(nff // LANES):
            cden[pl.ds(IN_ROW + IN_STEP * k + q, 1), :] = ci_v[pl.ds(k, 1), pl.ds(q * LANES, LANES)]
        rest = nff % LANES
        if rest:
            cden[pl.ds(IN_ROW + IN_STEP * k + nff // LANES, 1), pl.ds(0, rest)] = (
                ci_v[pl.ds(k, 1), pl.ds(nff - rest, rest)])
    for k in range(nk):
        vec = ri_v[pl.ds(k, 1), :]
        for p in range(0, ni, LANES):
            n = min(LANES, ni - p)
            rcol[pl.ds(k * ni + p, n), :] = lane_to_column(vec[:, p:p + n], n)
    vec = ro_v[...]
    for p in range(0, no, LANES):
        n = min(LANES, no - p)
        rows = -(-n // 8) * 8
        rcol[pl.ds(nk * ni + p, rows), :] = lane_to_column(vec[:, p:p + n], rows)
    rsum[...] = jnp.broadcast_to(jnp.sum(rsum[...], axis=1, keepdims=True), rsum.shape)
    back_stage(1)

    def w_square_in(k):
        def body(q, acc):
            w = wi[k, :, pl.ds(pl.multiple_of(q * LANES, LANES), LANES)]
            return acc + w * w
        acc = lax.fori_loop(0, nff // LANES, body, jnp.zeros((ni, LANES), F32), unroll=4)
        rest = nff % LANES
        w = wi[k, :, pl.ds(nff - rest, rest)]
        return total(acc) + total(w * w)

    def w_square_out():
        m = no // 8 * 8
        acc = jnp.zeros((8, nd), F32)
        acc = lax.fori_loop(0, m // 8, lambda i, a: a + jnp.square(wo[pl.ds(pl.multiple_of(i * 8, 8), 8), :]), acc,
                            unroll=4)
        w = wo[pl.ds(m, no - m), :]
        return total(acc) + total(w * w)

    scope("wsq")
    w_sq = []
    for k in range(nk):
        w_cp[k].wait()
        w_sq.append(w_square_in(k))
    scope("back2")
    back_stage(2)
    scope("wsq2")
    w_cp[nk].wait()
    w_sq.append(w_square_out())
    back_stage(3)

    scope("wait1")
    for g in range(len(STAGED)):
        ref = tot.at[halves(*STAGED[g], 1 - core), :]
        bytes_of(ref, back_sem.at[g, 1])
    for g in range(len(DIRECT)):
        start, size = DIRECT[g]
        rows = pl.ds(start - DIRECT_ROW, size)
        bytes_of(recv_all.at[pl.ds(0, n_dev - 1), rows, :], all_sem.at[g, 1])
    t = recv_all[0]
    for c in range(1, n_dev):
        t = t + recv_all[c]
    tot[pl.ds(DIRECT_ROW, t.shape[0]), :] = t

    scope("stats")
    beta = jnp.full((1, 1), beta_s[()], F32)
    mix = 1.0 - beta
    seg = [(IN_ROW + IN_STEP * k, IN_STEP, k * ni, ni, rows_in, nff) for k in range(nk)]
    seg.append((OUT_ROW, SCALAR_ROW, nk * ni, no_pad, rows_out, nd))
    sums = [total(tot[pl.ds(a, n), :]) for a, n, *_ in seg]
    norm_sq = sums[0] + sums[1] + sums[2]
    scale = jnp.minimum(1.0, jnp.full((1, 1), cnorm_s[()], F32) / jnp.sqrt(norm_sq))
    row_tot = tot[pl.ds(SCALAR_ROW, 1), :]
    for j, (a, n, ra, rn, m_all, n_all) in enumerate(seg):
        c2 = beta * cden[pl.ds(a, n), :] + mix * (scale * (scale * tot[pl.ds(a, n), :]) * (1.0 / m_all) + EPS_ONE)
        cnew[pl.ds(a, n), :] = c2
        bden[pl.ds(a, n), :] = scale * lax.rsqrt(c2)
        r2 = beta * rcol[pl.ds(ra, rn), :] + mix * (scale * (scale * rsum[pl.ds(ra, rn), :]) * (1.0 / n_all) + EPS_ONE)
        rcol[pl.ds(ra, rn), :] = r2
        r_all = jnp.sum(jnp.where(lane == j, row_tot, 0.0), axis=1, keepdims=True)
        level = beta * (r_all / m_all) + mix * (scale * (scale * (sums[j] / n_all)) * (1.0 / m_all) + EPS_ONE)
        acol[pl.ds(ra, rn), :] = lax.rsqrt(r2 / level)

    def u_square(ref, k, row0, m, cols, stat0, arow, unroll):
        rows = pl.ds(row0, m)

        def block(col, w, brow):
            idx = (rows, pl.ds(col, w)) if k is None else (k, rows, pl.ds(col, w))
            t = ref[idx] * jnp.broadcast_to(bden[pl.ds(brow, 1), pl.ds(0, w)], (m, w))
            return t * t

        def body(i, acc):
            for q in range(unroll):
                col = pl.multiple_of((i * unroll + q) * LANES, LANES)
                acc = acc + block(col, LANES, stat0 + i * unroll + q)
            return acc
        acc = lax.fori_loop(0, cols // LANES // unroll, body, jnp.zeros((m, LANES), F32))
        a = acol[pl.ds(arow, m), :]
        u = total(acc * a * a)
        rest = cols % LANES
        if rest:
            a = acol[pl.ds(arow, m), pl.ds(0, rest)]
            u = u + total(block(cols - rest, rest, stat0 + cols // LANES) * a * a)
        return u

    scope("upass")
    u_sq = [u_square(di, k, 0, ni, nff, IN_ROW + IN_STEP * k, k * ni, 13) for k in range(nk)]
    u_sq.append(sum(u_square(do, None, row0, m, nd, OUT_ROW, nk * ni + row0, 10)
                    for row0, m in ((0, 144), (144, 144), (288, no - 288))))

    scope("x2")
    msg = jnp.zeros((1, LANES), F32)
    for j in range(3):
        msg = msg + jnp.where(lane == j, u_sq[j], 0.0) + jnp.where(lane == 3 + j, w_sq[j], 0.0)
    recv2[me] = msg
    for d in range(1, n_dev):
        two_copy(d).start()
    for g in range(len(STAGED)):
        pair_copy(g).wait_send()
        back_copy(g).wait_send()
        bytes_of(recv.at[pl.ds(0, n_chip - 1), halves(*STAGED[g], core), :], chip_sem.at[g, 0])
    for g in range(len(DIRECT)):
        start, size = DIRECT[g]
        bytes_of(recv_all.at[pl.ds(0, n_dev - 1), pl.ds(start - DIRECT_ROW, size), :], all_sem.at[g, 0])
    bytes_of(recv2.at[pl.ds(0, n_dev - 1)], two_sem.at[1])
    scope("fin")
    all_sums = recv2[0]
    for c in range(1, n_dev):
        all_sums = all_sums + recv2[c]
    for j, (_, _, _, _, m_all, n_all) in enumerate(seg):
        u = jnp.sum(jnp.where(lane == j, all_sums, 0.0), axis=1, keepdims=True)
        w = jnp.sum(jnp.where(lane == 3 + j, all_sums, 0.0), axis=1, keepdims=True)
        u_rms = jnp.sqrt(u / (m_all * n_all))
        w_rms = jnp.sqrt(w / (m_all * n_all))
        step_size = jnp.full((1, 1), rel_s[()], F32) * jnp.maximum(EPS_TWO, w_rms)
        k = step_size / jnp.maximum(1.0, u_rms / jnp.full((1, 1), crms_s[()], F32))
        kout[pl.ds(j, 1), :] = jnp.broadcast_to(k, (1, LANES))
    bytes_of(recv2.at[pl.ds(0, n_dev - 1)], two_sem.at[0])
    scope(None)


B_IN = 32


def update_kernel(di, do, wi, wo, rcol, acol, cnew, bden, kout, wi_out, ri_hbm, ci_hbm, wo_out, ro_hbm, co_hbm,
                  buf_in, buf_out, sem_in, sem_out, ri_out, ci_out, ro_out, co_out, sem_small):
    nk, ni, nff = di.shape
    no, nd = do.shape
    steps = ni // B_IN

    def in_copy(k, i, slot):
        return pltpu.make_async_copy(buf_in.at[slot], wi_out.at[k, pl.ds(i * B_IN, B_IN), :], sem_in.at[slot])

    def widths(n):
        return [(c, min(LANES, n - c)) for c in range(0, n, LANES)]

    def step_of(w, g, b, a, kk):
        return w - kk * ((g * jnp.broadcast_to(b, g.shape)) * a)

    scope("u_in")
    pend = [None] * buf_in.shape[0]
    for k in range(nk):
        kk = jnp.broadcast_to(kout[pl.ds(k, 1), :], (B_IN, LANES))
        for i in range(steps):
            slot = (k * steps + i) % buf_in.shape[0]
            if pend[slot] is not None:
                pend[slot].wait()
            a = acol[pl.ds(k * ni + i * B_IN, B_IN), :]
            rows = pl.ds(i * B_IN, B_IN)
            for q, (c, n) in enumerate(widths(nff)):
                cc = pl.ds(c, n)
                b = bden[pl.ds(IN_ROW + IN_STEP * k + q, 1), pl.ds(0, n)]
                buf_in[slot, :, cc] = step_of(wi[k, rows, cc], di[k, rows, cc], b, a[:, :n], kk[:, :n])
            cp = in_copy(k, i, slot)
            cp.start()
            pend[slot] = cp
    scope("u_small")
    co_out[...] = cnew[pl.ds(OUT_ROW, nd // LANES), :]
    for k in range(nk):
        for c, n in widths(nff):
            ci_out[pl.ds(k, 1), pl.ds(c, n)] = cnew[pl.ds(IN_ROW + IN_STEP * k + c // LANES, 1), pl.ds(0, n)]
        for c, n in widths(ni):
            ri_out[pl.ds(k, 1), pl.ds(c, n)] = column_to_lane(rcol[pl.ds(k * ni + c, n), :], n)
    for c, n in widths(no):
        ro_out[:, pl.ds(c, n)] = column_to_lane(rcol[pl.ds(nk * ni + c, -(-n // 8) * 8), :], n)
    small = [pltpu.make_async_copy(v, h, sem_small.at[i]) for i, (v, h) in enumerate(
        ((ri_out, ri_hbm), (ci_out, ci_hbm), (ro_out, ro_hbm), (co_out, co_hbm)))]
    for cp in small:
        cp.start()
    scope("u_out")
    pend_out = [None] * buf_out.shape[0]
    for i in range(nd // CHUNK):
        slot = i % buf_out.shape[0]
        if pend_out[slot] is not None:
            pend_out[slot].wait()
        kk = jnp.broadcast_to(kout[pl.ds(nk, 1), :], (40, LANES))
        bs = [bden[pl.ds(OUT_ROW + i * (CHUNK // LANES) + q, 1), :] for q in range(CHUNK // LANES)]

        def rows_of(o, n, i=i, slot=slot, kk=kk, bs=bs):
            r = pl.ds(o, n)
            a = acol[pl.ds(nk * ni + o, n), :]
            for q, b in enumerate(bs):
                cc = pl.ds(i * CHUNK + q * LANES, LANES)
                buf_out[slot, r, pl.ds(q * LANES, LANES)] = step_of(wo[r, cc], do[r, cc], b, a, kk[:n])

        for o in range(0, no, 40):
            rows_of(o, min(40, no - o))
        cp = pltpu.make_async_copy(buf_out.at[slot], wo_out.at[:, pl.ds(i * CHUNK, CHUNK)], sem_out.at[slot])
        cp.start()
        pend_out[slot] = cp
    scope("u_wait")
    for cp in pend + pend_out + small:
        if cp is not None:
            cp.wait()
    scope(None)


def solution(mesh):
    n_dev = mesh.shape['tp']

    def local_step(x_norm, hid_act, dy_in, dy_out, w_in, w_out, row_in, col_in, row_out, col_out,
                   beta_two, rel_step, clip_rms, clip_norm):
        t, ni = x_norm.shape
        no = hid_act.shape[1]
        nk, _, nff = dy_in.shape
        nd = dy_out.shape[1]
        no_pad = -(-no // 8) * 8
        tail_cols = nff - nff // SUPER * SUPER
        vm = pl.BlockSpec(memory_space=pltpu.VMEM)
        hb = pl.BlockSpec(memory_space=pltpu.HBM)
        sm = pl.BlockSpec(memory_space=pltpu.SMEM)
        dma = pltpu.SemaphoreType.DMA
        n_rows = nk * ni + no_pad
        a_out = [pltpu.VMEM((nk, ni, nff), F32), pltpu.VMEM((no, nd), F32),
                 pltpu.VMEM((nk, ni, nff), F32), pltpu.VMEM((no, nd), F32),
                 pltpu.VMEM((n_rows, LANES), F32), pltpu.VMEM((n_rows, LANES), F32),
                 pltpu.VMEM((STAT_ROWS, LANES), F32), pltpu.VMEM((STAT_ROWS, LANES), F32),
                 pltpu.VMEM((8, LANES), F32)]
        ns, ng = len(STAGED), len(DIRECT)
        stat = pltpu.VMEM((STAT_ROWS, LANES), F32)
        outs = pl.pallas_call(
            lambda *refs: stats_kernel(n_dev, *refs),
            out_shape=a_out,
            in_specs=[hb] * 10 + [sm] * 4,
            out_specs=[vm] * len(a_out),
            scratch_shapes=[
                pltpu.VMEM((ni, t), BF16), pltpu.VMEM((no, t), BF16), pltpu.VMEM((t, nd), BF16),
                pltpu.VMEM((SLOTS, SUPER, t), BF16), pltpu.VMEM((nk, tail_cols, t), BF16), pltpu.VMEM((2, 256, ni), F32),
                pltpu.VMEM((nk, ni), F32), pltpu.VMEM((nk, nff), F32), pltpu.VMEM((1, no), F32),
                pltpu.VMEM((nd // LANES, LANES), F32),
                stat, stat, stat, pltpu.VMEM((n_dev // 2, STAT_ROWS, LANES), F32),
                pltpu.VMEM((n_dev, sum(n for _, n in DIRECT), LANES), F32), stat,
                pltpu.VMEM((n_rows, LANES), F32), pltpu.VMEM((n_dev, 1, LANES), F32),
                dma((6,)), dma((nd // CHUNK,)), dma((SLOTS, 2)), dma((nk,)), dma((nk + 1,)),
                dma((ns, 2)), dma((ns, 2)), dma((ns, 2)), dma((ng, 2)), dma((2,)),
            ],
            compiler_params=pltpu.CompilerParams(collective_id=0, has_side_effects=True,
                                                 vmem_limit_bytes=SCOPED),
            name="stats",
        )(x_norm.T, hid_act.T, dy_out, jnp.swapaxes(dy_in, 1, 2), w_in, w_out, row_in, col_in,
          row_out.reshape(1, no), col_out.reshape(nd // LANES, LANES),
          beta_two, rel_step, clip_rms, clip_norm)
        outs = [pltpu.with_memory_space_constraint(o, pltpu.VMEM) for o in outs]
        b_out = [jax.ShapeDtypeStruct(w_in.shape, F32), jax.ShapeDtypeStruct(row_in.shape, F32),
                 jax.ShapeDtypeStruct(col_in.shape, F32), jax.ShapeDtypeStruct(w_out.shape, F32),
                 jax.ShapeDtypeStruct((1, no), F32), jax.ShapeDtypeStruct((nd // LANES, LANES), F32)]
        wi_new, ri_new, ci_new, wo_new, ro_new, co_new = pl.pallas_call(
            update_kernel,
            out_shape=b_out,
            in_specs=[vm] * len(outs),
            out_specs=[hb] * 6,
            scratch_shapes=[pltpu.VMEM((nk * ni // B_IN, B_IN, nff), F32), pltpu.VMEM((nd // CHUNK, no, CHUNK), F32),
                            dma((nk * ni // B_IN,)), dma((nd // CHUNK,)),
                            pltpu.VMEM((nk, ni), F32), pltpu.VMEM((nk, nff), F32), pltpu.VMEM((1, no), F32),
                            pltpu.VMEM((nd // LANES, LANES), F32), dma((4,))],
            compiler_params=pltpu.CompilerParams(vmem_limit_bytes=SCOPED),
            name="update",
        )(*outs)
        return (wi_new, ri_new, ci_new, wo_new, ro_new.reshape(no), co_new.reshape(nd))

    in_specs = (P(None, 'tp'), P(None, 'tp'), P(), P(), P(None, 'tp', None), P('tp', None),
                P(None, 'tp'), P(), P('tp'), P(), P(), P(), P(), P())
    out_specs = (P(None, 'tp', None), P(None, 'tp'), P(), P('tp', None), P('tp'), P())
    return jax.shard_map(local_step, mesh=mesh, in_specs=in_specs, out_specs=out_specs, check_vma=False)
```

```python
import jax
import jax.numpy as jnp
from jax import lax
from jax.experimental import pallas as pl
from jax.experimental.pallas import tpu as pltpu
from jax.sharding import PartitionSpec as P

MESH = pl.DeviceIdType.MESH
EPS_ONE = 1e-30
EPS_TWO = 1e-3
LANES = 128
F32 = jnp.float32
BF16 = jnp.bfloat16

OUT_ROW, IN_ROW, IN_STEP, STAT_ROWS = 0, 32, 64, 160
SCALAR_ROW = 24
STAGED = ((0, 32), (32, 64), (128, 32), (112, 16))
DIRECT_ROW = 96
DIRECT = ((96, 8), (104, 8))
CHUNK = 512
SUPER = 2048
HALF = 1024
SLOTS = 4
SCOPED = 30 * 1024 * 1024
PIECE = 256


def scope(name):
    pass


def lane_to_column(vec, rows):
    n = vec.shape[1]
    r = lax.broadcasted_iota(jnp.int32, (rows, n), 0)
    c = lax.broadcasted_iota(jnp.int32, (rows, n), 1)
    col = jnp.sum(jnp.where(r == c, jnp.broadcast_to(vec, (rows, n)), 0.0), axis=1, keepdims=True)
    full = jnp.broadcast_to(col, (rows, LANES))
    if rows > n:
        full = jnp.where(lax.broadcasted_iota(jnp.int32, (rows, LANES), 0) < n, full, 1.0)
    return full


def column_to_lane(col, n):
    part = col[:, :n]
    r = lax.broadcasted_iota(jnp.int32, part.shape, 0)
    c = lax.broadcasted_iota(jnp.int32, part.shape, 1)
    return jnp.sum(jnp.where(r == c, part, 0.0), axis=0, keepdims=True)


def total(x):
    return jnp.sum(jnp.sum(x, axis=0, keepdims=True), axis=1, keepdims=True)


def stats_kernel(n_dev, x_hbm, h_hbm, dyo_hbm, dyi_hbm, wi_hbm, wo_hbm, ri_hbm, ci_hbm, ro_hbm, co_hbm,
                 beta_s, rel_s, crms_s, cnorm_s,
                 di, do, wi, wo, rcol, acol, cnew, bden, kout,
                 x_v, h_v, dyo_v, ring, tail, raw, turned, ri_v, ci_v, ro_v, co_v, part, pair, tot, recv, recv_all, cden, rsum, recv2,
                 in_sem, dyo_sem, ring_sem, tail_sem, w_sem, pair_sem, chip_sem, back_sem, all_sem, two_sem):
    me = lax.axis_index('tp')
    core = lax.rem(me, 2)
    chip = me // 2
    partner = me + 1 - 2 * core
    nk, ni, nff = di.shape
    no, nd = wo.shape
    no_pad = -(-no // 8) * 8
    n_super = nff // SUPER
    tail_cols = nff - n_super * SUPER
    rows_in, rows_out = ni * n_dev, no * n_dev
    n_chip = n_dev // 2

    barrier = pltpu.get_barrier_semaphore()
    for d in range(1, n_dev):
        pl.semaphore_signal(barrier, inc=1, device_id=(lax.rem(me + d, n_dev),), device_id_type=MESH)

    scope("init")
    sequence = [(0, c) for c in range(n_super)] + [(1, c) for c in range(n_super - 1, -1, -1)]

    def half_copy(i, p):
        k, c = sequence[i]
        return pltpu.make_async_copy(dyi_hbm.at[k, pl.ds(c * SUPER + p * HALF, HALF), :],
                                     ring.at[i % SLOTS, pl.ds(p * HALF, HALF), :], ring_sem.at[i % SLOTS, p])

    def super_start(i):
        half_copy(i, 0).start()
        half_copy(i, 1).start()

    def super_wait(i):
        half_copy(i, 0).wait()
        half_copy(i, 1).wait()

    tail_cp = [pltpu.make_async_copy(dyi_hbm.at[k, pl.ds(n_super * SUPER, tail_cols), :], tail.at[k], tail_sem.at[k])
               for k in range(nk)]
    w_cp = [pltpu.make_async_copy(wi_hbm.at[k], wi.at[k], w_sem.at[k]) for k in range(nk)]
    w_cp.append(pltpu.make_async_copy(wo_hbm, wo, w_sem.at[nk]))
    small = [pltpu.make_async_copy(a, b, in_sem.at[i]) for i, (a, b) in enumerate(
        ((ro_hbm, ro_v), (ri_hbm, ri_v), (co_hbm, co_v), (ci_hbm, ci_v), (h_hbm, h_v), (x_hbm, x_v)))]
    dyo_cp = [pltpu.make_async_copy(dyo_hbm.at[:, pl.ds(c, CHUNK)], dyo_v.at[:, pl.ds(c, CHUNK)],
                                    dyo_sem.at[c // CHUNK]) for c in range(0, nd, CHUNK)]
    for cp in small[4:5] + dyo_cp[:1]:
        cp.start()
    part[...] = jnp.zeros_like(part)
    rsum[...] = jnp.zeros_like(rsum)
    dyo_cp[1].start()

    def halves(start, size, c):
        return pl.ds(pl.multiple_of(start + c * (size // 2), 8), size // 2)

    def remote(src, dst, sem, device):
        return pltpu.make_async_remote_copy(src_ref=src, dst_ref=dst, send_sem=sem.at[0], recv_sem=sem.at[1],
                                            device_id=(device,), device_id_type=MESH)

    def pair_copy(g):
        rows = halves(*STAGED[g], 1 - core)
        return remote(part.at[rows, :], pair.at[rows, :], pair_sem.at[g], partner)

    def chip_copy(g, d):
        ref = recv.at[chip, halves(*STAGED[g], core), :]
        return remote(ref, ref, chip_sem.at[g], lax.rem(me + 2 * d, n_dev))

    def back_copy(g):
        ref = tot.at[halves(*STAGED[g], core), :]
        return remote(ref, ref, back_sem.at[g], partner)

    def all_copy(g, d):
        start, size = DIRECT[g]
        ref = recv_all.at[me, pl.ds(start - DIRECT_ROW, size), :]
        return remote(ref, ref, all_sem.at[g], lax.rem(me + d, n_dev))

    def two_copy(d):
        return remote(recv2.at[me], recv2.at[me], two_sem, lax.rem(me + d, n_dev))

    def bytes_of(ref, sem):
        pltpu.make_async_copy(ref, ref, sem).wait()

    def chip_stage(g):
        rows = halves(*STAGED[g], core)
        pair_copy(g).wait_recv()
        recv[chip, rows, :] = part[rows, :] + pair[rows, :]
        for d in range(1, n_chip):
            chip_copy(g, d).start()

    def back_stage(g):
        start, size = STAGED[g]
        rows = halves(start, size, core)
        bytes_of(recv.at[pl.ds(0, n_chip - 1), rows, :], chip_sem.at[g, 1])
        t = recv[0, rows, :]
        for c in range(1, n_chip):
            t = t + recv[c, rows, :]
        tot[rows, :] = t
        back_copy(g).start()

    def direct_stage(g):
        start, size = DIRECT[g]
        rows = pl.ds(start - DIRECT_ROW, size)
        recv_all[me, rows, :] = part[pl.ds(start, size), :]
        for d in range(1, n_dev):
            all_copy(g, d).start()

    def square_sums(g, row0, stat0):
        m, n = g.shape
        sq = g * g
        cols = jnp.sum(sq, axis=0, keepdims=True)
        acc = rsum[pl.ds(row0, m), :]
        for b in range(0, n, LANES):
            w = min(LANES, n - b)
            if w == LANES:
                acc += sq[:, b:b + w]
                part[pl.ds(stat0 + b // LANES, 1), :] = cols[:, b:b + w]
            else:
                acc = acc + jnp.concatenate([sq[:, b:b + w], jnp.zeros((m, LANES - w), F32)], axis=1)
                part[pl.ds(stat0 + b // LANES, 1), pl.ds(0, w)] = cols[:, b:b + w]
        rsum[pl.ds(row0, m), :] = acc

    deferred = []

    def flush():
        for f in deferred:
            f()
        deferred.clear()

    def finish_in(k, col, g, store):
        if store:
            di[k, :, pl.ds(col, g.shape[1])] = g
        square_sums(g, k * ni, IN_ROW + IN_STEP * k + col // LANES)

    def finish_out(col):
        square_sums(do[:, pl.ds(col, 256)], nk * ni, OUT_ROW + col // LANES)

    def in_block(pieces, defer):
        for j, (k, col, n, ref) in enumerate(pieces):
            slot = j - len(pieces) + 2
            defer_this = defer and slot >= 0
            if j%2==1:
                turned[j % 4, :, pl.ds(0, n)] = ref[...].T
                g = jnp.dot(x_v[...], turned[j % 4, :, pl.ds(0, n)], preferred_element_type=F32)
                if defer_this:
                    di[k, :, pl.ds(col, n)] = g
                    deferred.append(lambda k=k, col=col, n=n: finish_in(k, col, di[k, :, pl.ds(col, n)], False))
                else:
                    finish_in(k, col, g, True)
            else:
                g = lax.dot_general(ref[...], x_v[...], (((1,), (1,)), ((), ())), preferred_element_type=F32)
                if defer_this:
                    raw[slot, pl.ds(0, n), :] = g
                    deferred.append(lambda k=k, col=col, n=n, slot=slot:
                                    finish_in(k, col, raw[slot, pl.ds(0, n), :].T, True))
                else:
                    finish_in(k, col, g.T, True)

    def super_pieces(i, start=0, stop=SUPER):
        k, c = sequence[i]
        return [(k, c * SUPER + p, 256, ring.at[i % SLOTS, pl.ds(p, 256), :]) for p in range(start, stop, 256)]

    def tail_pieces(k):
        return [(k, n_super * SUPER + p, min(256, tail_cols - p), tail.at[k, pl.ds(p, min(256, tail_cols - p)), :])
                for p in range(0, tail_cols, 256)]

    def out_piece(start, stop):
        for col in range(start, stop, 256):
            do[:, pl.ds(col, 256)] = jnp.dot(h_v[...], dyo_v[:, pl.ds(col, 256)], preferred_element_type=F32)
            if col + 512 >= stop:
                deferred.append(lambda col=col: finish_out(col))
            else:
                finish_out(col)

    scope("out")
    small[4].wait()
    dyo_cp[0].wait()
    for cp in dyo_cp[2:4]:
        cp.start()
    out_piece(0, CHUNK)
    dyo_cp[1].wait()
    for cp in dyo_cp[4:] + small[5:6] + small[:4]:
        cp.start()
    half_copy(0, 0).start()
    scope("out1")
    dyo_cp[2].wait()
    flush()
    out_piece(CHUNK, 3 * CHUNK)
    half_copy(0, 1).start()
    super_start(1)
    scope("out2")
    for cp in dyo_cp[3:]:
        cp.wait()
    flush()
    out_piece(3 * CHUNK, nd)
    for cp in small[:2]:
        cp.wait()
    lane = lax.broadcasted_iota(jnp.int32, (1, LANES), 1)
    row_sums = jnp.where(lane == 2, jnp.sum(ro_v[...], axis=1, keepdims=True), 0.0)
    for k in range(nk):
        row_sums += jnp.where(lane == k, jnp.sum(ri_v[pl.ds(k, 1), :], axis=1, keepdims=True), 0.0)
    part[pl.ds(SCALAR_ROW, 1), :] = row_sums
    scope("in0")
    small[5].wait()
    super_wait(0)
    super_start(2)
    tail_cp[0].start()
    flush()
    in_block(super_pieces(0), False)
    pl.semaphore_wait(barrier, n_dev - 1)
    pair_copy(0).start()
    scope("in1")
    super_wait(1)
    super_start(3)
    tail_cp[1].start()
    flush()
    in_block(super_pieces(1), False)
    chip_stage(0)
    scope("in2")
    super_wait(2)
    tail_cp[0].wait()
    super_start(4)
    flush()
    in_block(super_pieces(2) + tail_pieces(0), False)
    pair_copy(1).start()
    scope("in3")
    super_wait(3)
    tail_cp[1].wait()
    super_start(5)
    in_block(super_pieces(3) + tail_pieces(1), False)
    pair_copy(2).start()
    chip_stage(1)
    scope("in4")
    super_wait(4)
    w_cp[0].start()
    in_block(super_pieces(4), False)
    pair_copy(3).start()
    chip_stage(2)
    scope("in5")
    super_wait(5)
    for cp in w_cp[1:]:
        cp.start()
    in_block(super_pieces(5, 0, HALF), False)
    direct_stage(0)
    chip_stage(3)
    in_block(super_pieces(5, HALF, SUPER), False)
    direct_stage(1)
    back_stage(0)

    scope("forms")
    for cp in small[2:4]:
        cp.wait()
    cden[...] = jnp.ones_like(cden)
    cden[pl.ds(OUT_ROW, nd // LANES), :] = co_v[...]
    for k in range(nk):
        for q in range(nff // LANES):
            cden[pl.ds(IN_ROW + IN_STEP * k + q, 1), :] = ci_v[pl.ds(k, 1), pl.ds(q * LANES, LANES)]
        rest = nff % LANES
        if rest:
            cden[pl.ds(IN_ROW + IN_STEP * k + nff // LANES, 1), pl.ds(0, rest)] = (
                ci_v[pl.ds(k, 1), pl.ds(nff - rest, rest)])
    for k in range(nk):
        vec = ri_v[pl.ds(k, 1), :]
        for p in range(0, ni, LANES):
            n = min(LANES, ni - p)
            rcol[pl.ds(k * ni + p, n), :] = lane_to_column(vec[:, p:p + n], n)
    vec = ro_v[...]
    for p in range(0, no, LANES):
        n = min(LANES, no - p)
        rows = -(-n // 8) * 8
        rcol[pl.ds(nk * ni + p, rows), :] = lane_to_column(vec[:, p:p + n], rows)
    rsum[...] = jnp.broadcast_to(jnp.sum(rsum[...], axis=1, keepdims=True), rsum.shape)
    back_stage(1)

    def w_square_in(k):
        def body(q, acc):
            w = wi[k, :, pl.ds(pl.multiple_of(q * LANES, LANES), LANES)]
            return acc + w * w
        acc = lax.fori_loop(0, nff // LANES, body, jnp.zeros((ni, LANES), F32), unroll=4)
        rest = nff % LANES
        w = wi[k, :, pl.ds(nff - rest, rest)]
        return total(acc) + total(w * w)

    def w_square_out():
        m = no // 8 * 8
        acc = jnp.zeros((8, nd), F32)
        acc = lax.fori_loop(0, m // 8, lambda i, a: a + jnp.square(wo[pl.ds(pl.multiple_of(i * 8, 8), 8), :]), acc,
                            unroll=4)
        w = wo[pl.ds(m, no - m), :]
        return total(acc) + total(w * w)

    scope("wsq")
    w_sq = []
    for k in range(nk):
        w_cp[k].wait()
        w_sq.append(w_square_in(k))
    scope("back2")
    back_stage(2)
    scope("wsq2")
    w_cp[nk].wait()
    w_sq.append(w_square_out())
    back_stage(3)

    scope("wait1")
    for g in range(len(STAGED)):
        ref = tot.at[halves(*STAGED[g], 1 - core), :]
        bytes_of(ref, back_sem.at[g, 1])
    for g in range(len(DIRECT)):
        start, size = DIRECT[g]
        rows = pl.ds(start - DIRECT_ROW, size)
        bytes_of(recv_all.at[pl.ds(0, n_dev - 1), rows, :], all_sem.at[g, 1])
    t = recv_all[0]
    for c in range(1, n_dev):
        t = t + recv_all[c]
    tot[pl.ds(DIRECT_ROW, t.shape[0]), :] = t

    scope("stats")
    beta = jnp.full((1, 1), beta_s[()], F32)
    mix = 1.0 - beta
    seg = [(IN_ROW + IN_STEP * k, IN_STEP, k * ni, ni, rows_in, nff) for k in range(nk)]
    seg.append((OUT_ROW, SCALAR_ROW, nk * ni, no_pad, rows_out, nd))
    sums = [total(tot[pl.ds(a, n), :]) for a, n, *_ in seg]
    norm_sq = sums[0] + sums[1] + sums[2]
    scale = jnp.minimum(1.0, jnp.full((1, 1), cnorm_s[()], F32) / jnp.sqrt(norm_sq))
    row_tot = tot[pl.ds(SCALAR_ROW, 1), :]
    for j, (a, n, ra, rn, m_all, n_all) in enumerate(seg):
        c2 = beta * cden[pl.ds(a, n), :] + mix * (scale * (scale * tot[pl.ds(a, n), :]) * (1.0 / m_all) + EPS_ONE)
        cnew[pl.ds(a, n), :] = c2
        bden[pl.ds(a, n), :] = scale * lax.rsqrt(c2)
        r2 = beta * rcol[pl.ds(ra, rn), :] + mix * (scale * (scale * rsum[pl.ds(ra, rn), :]) * (1.0 / n_all) + EPS_ONE)
        rcol[pl.ds(ra, rn), :] = r2
        r_all = jnp.sum(jnp.where(lane == j, row_tot, 0.0), axis=1, keepdims=True)
        level = beta * (r_all / m_all) + mix * (scale * (scale * (sums[j] / n_all)) * (1.0 / m_all) + EPS_ONE)
        acol[pl.ds(ra, rn), :] = lax.rsqrt(r2 / level)

    def u_square(ref, k, row0, m, cols, stat0, arow):
        rows = pl.ds(row0, m)

        def block(col, w, brow):
            idx = (rows, pl.ds(col, w)) if k is None else (k, rows, pl.ds(col, w))
            t = ref[idx] * jnp.broadcast_to(bden[pl.ds(brow, 1), pl.ds(0, w)], (m, w))
            return t * t

        acc = jnp.zeros((m, LANES), F32)
        for q in range(cols // LANES):
            acc = acc + block(q * LANES, LANES, stat0 + q)
        a = acol[pl.ds(arow, m), :]
        u = jnp.sum(acc * a * a, axis=0, keepdims=True)
        rest = cols % LANES
        if rest:
            a = acol[pl.ds(arow, m), pl.ds(0, rest)]
            r = jnp.sum(block(cols - rest, rest, stat0 + cols // LANES) * a * a, axis=0, keepdims=True)
            u = u + jnp.concatenate([r, jnp.zeros((1, LANES - rest), F32)], axis=1)
        return u

    scope("upass")
    u_sq = [u_square(di, k, 0, ni, nff, IN_ROW + IN_STEP * k, k * ni) for k in range(nk)]
    u_sq.append(sum(u_square(do, None, row0, m, nd, OUT_ROW, nk * ni + row0)
                    for row0, m in ((0, 144), (144, 144), (288, no - 288))))

    scope("x2")
    msg = jnp.zeros((1, LANES), F32)
    for j in range(3):
        msg = msg + jnp.where(lane == j, jnp.sum(u_sq[j], axis=1, keepdims=True), 0.0) + jnp.where(lane == 3 + j, w_sq[j], 0.0)
    recv2[me] = msg
    for d in range(1, n_dev):
        two_copy(d).start()
    for g in range(len(STAGED)):
        pair_copy(g).wait_send()
        back_copy(g).wait_send()
        bytes_of(recv.at[pl.ds(0, n_chip - 1), halves(*STAGED[g], core), :], chip_sem.at[g, 0])
    for g in range(len(DIRECT)):
        start, size = DIRECT[g]
        bytes_of(recv_all.at[pl.ds(0, n_dev - 1), pl.ds(start - DIRECT_ROW, size), :], all_sem.at[g, 0])
    bytes_of(recv2.at[pl.ds(0, n_dev - 1)], two_sem.at[1])
    scope("fin")
    all_sums = recv2[0]
    for c in range(1, n_dev):
        all_sums = all_sums + recv2[c]
    for j, (_, _, _, _, m_all, n_all) in enumerate(seg):
        u = jnp.sum(jnp.where(lane == j, all_sums, 0.0), axis=1, keepdims=True)
        w = jnp.sum(jnp.where(lane == 3 + j, all_sums, 0.0), axis=1, keepdims=True)
        u_rms = jnp.sqrt(u / (m_all * n_all))
        w_rms = jnp.sqrt(w / (m_all * n_all))
        step_size = jnp.full((1, 1), rel_s[()], F32) * jnp.maximum(EPS_TWO, w_rms)
        k = step_size / jnp.maximum(1.0, u_rms / jnp.full((1, 1), crms_s[()], F32))
        kout[pl.ds(j, 1), :] = jnp.broadcast_to(k, (1, LANES))
    bytes_of(recv2.at[pl.ds(0, n_dev - 1)], two_sem.at[0])
    scope(None)


B_IN = 32


def update_kernel(di, do, wi, wo, rcol, acol, cnew, bden, kout, wi_out, ri_hbm, ci_hbm, wo_out, ro_hbm, co_hbm,
                  buf_in, buf_out, sem_in, sem_out, ri_out, ci_out, ro_out, co_out, sem_small):
    nk, ni, nff = di.shape
    no, nd = do.shape
    steps = ni // B_IN

    def in_copy(k, i, slot):
        return pltpu.make_async_copy(buf_in.at[slot], wi_out.at[k, pl.ds(i * B_IN, B_IN), :], sem_in.at[slot])

    def widths(n):
        return [(c, min(LANES, n - c)) for c in range(0, n, LANES)]

    def step_of(w, g, b, a, kk):
        return w - kk * ((g * jnp.broadcast_to(b, g.shape)) * a)

    scope("u_in")
    pend = [None] * buf_in.shape[0]
    for k in range(nk):
        kk = jnp.broadcast_to(kout[pl.ds(k, 1), :], (B_IN, LANES))
        for i in range(steps):
            slot = (k * steps + i) % buf_in.shape[0]
            if pend[slot] is not None:
                pend[slot].wait()
            a = acol[pl.ds(k * ni + i * B_IN, B_IN), :]
            rows = pl.ds(i * B_IN, B_IN)
            for q, (c, n) in enumerate(widths(nff)):
                cc = pl.ds(c, n)
                b = bden[pl.ds(IN_ROW + IN_STEP * k + q, 1), pl.ds(0, n)]
                buf_in[slot, :, cc] = step_of(wi[k, rows, cc], di[k, rows, cc], b, a[:, :n], kk[:, :n])
            cp = in_copy(k, i, slot)
            cp.start()
            pend[slot] = cp
    scope("u_small")
    co_out[...] = cnew[pl.ds(OUT_ROW, nd // LANES), :]
    for k in range(nk):
        for c, n in widths(nff):
            ci_out[pl.ds(k, 1), pl.ds(c, n)] = cnew[pl.ds(IN_ROW + IN_STEP * k + c // LANES, 1), pl.ds(0, n)]
        for c, n in widths(ni):
            ri_out[pl.ds(k, 1), pl.ds(c, n)] = column_to_lane(rcol[pl.ds(k * ni + c, n), :], n)
    for c, n in widths(no):
        ro_out[:, pl.ds(c, n)] = column_to_lane(rcol[pl.ds(nk * ni + c, -(-n // 8) * 8), :], n)
    small = [pltpu.make_async_copy(v, h, sem_small.at[i]) for i, (v, h) in enumerate(
        ((ri_out, ri_hbm), (ci_out, ci_hbm), (ro_out, ro_hbm), (co_out, co_hbm)))]
    for cp in small:
        cp.start()
    scope("u_out")
    pend_out = [None] * buf_out.shape[0]
    for i in range(nd // CHUNK):
        slot = i % buf_out.shape[0]
        if pend_out[slot] is not None:
            pend_out[slot].wait()
        kk = jnp.broadcast_to(kout[pl.ds(nk, 1), :], (40, LANES))
        bs = [bden[pl.ds(OUT_ROW + i * (CHUNK // LANES) + q, 1), :] for q in range(CHUNK // LANES)]

        def rows_of(o, n, i=i, slot=slot, kk=kk, bs=bs):
            r = pl.ds(o, n)
            a = acol[pl.ds(nk * ni + o, n), :]
            for q, b in enumerate(bs):
                cc = pl.ds(i * CHUNK + q * LANES, LANES)
                buf_out[slot, r, pl.ds(q * LANES, LANES)] = step_of(wo[r, cc], do[r, cc], b, a, kk[:n])

        for o in range(0, no, 40):
            rows_of(o, min(40, no - o))
        cp = pltpu.make_async_copy(buf_out.at[slot], wo_out.at[:, pl.ds(i * CHUNK, CHUNK)], sem_out.at[slot])
        cp.start()
        pend_out[slot] = cp
    scope("u_wait")
    for cp in pend + pend_out + small:
        if cp is not None:
            cp.wait()
    scope(None)


def solution(mesh):
    n_dev = mesh.shape['tp']

    def local_step(x_norm, hid_act, dy_in, dy_out, w_in, w_out, row_in, col_in, row_out, col_out,
                   beta_two, rel_step, clip_rms, clip_norm):
        t, ni = x_norm.shape
        no = hid_act.shape[1]
        nk, _, nff = dy_in.shape
        nd = dy_out.shape[1]
        no_pad = -(-no // 8) * 8
        tail_cols = nff - nff // SUPER * SUPER
        vm = pl.BlockSpec(memory_space=pltpu.VMEM)
        hb = pl.BlockSpec(memory_space=pltpu.HBM)
        sm = pl.BlockSpec(memory_space=pltpu.SMEM)
        dma = pltpu.SemaphoreType.DMA
        n_rows = nk * ni + no_pad
        a_out = [pltpu.VMEM((nk, ni, nff), F32), pltpu.VMEM((no, nd), F32),
                 pltpu.VMEM((nk, ni, nff), F32), pltpu.VMEM((no, nd), F32),
                 pltpu.VMEM((n_rows, LANES), F32), pltpu.VMEM((n_rows, LANES), F32),
                 pltpu.VMEM((STAT_ROWS, LANES), F32), pltpu.VMEM((STAT_ROWS, LANES), F32),
                 pltpu.VMEM((8, LANES), F32)]
        ns, ng = len(STAGED), len(DIRECT)
        stat = pltpu.VMEM((STAT_ROWS, LANES), F32)
        outs = pl.pallas_call(
            lambda *refs: stats_kernel(n_dev, *refs),
            out_shape=a_out,
            in_specs=[hb] * 10 + [sm] * 4,
            out_specs=[vm] * len(a_out),
            scratch_shapes=[
                pltpu.VMEM((ni, t), BF16), pltpu.VMEM((no, t), BF16), pltpu.VMEM((t, nd), BF16),
                pltpu.VMEM((SLOTS, SUPER, t), BF16), pltpu.VMEM((nk, tail_cols, t), BF16), pltpu.VMEM((2, 256, ni), F32), pltpu.VMEM((4, t, 256), BF16),
                pltpu.VMEM((nk, ni), F32), pltpu.VMEM((nk, nff), F32), pltpu.VMEM((1, no), F32),
                pltpu.VMEM((nd // LANES, LANES), F32),
                stat, stat, stat, pltpu.VMEM((n_dev // 2, STAT_ROWS, LANES), F32),
                pltpu.VMEM((n_dev, sum(n for _, n in DIRECT), LANES), F32), stat,
                pltpu.VMEM((n_rows, LANES), F32), pltpu.VMEM((n_dev, 1, LANES), F32),
                dma((6,)), dma((nd // CHUNK,)), dma((SLOTS, 2)), dma((nk,)), dma((nk + 1,)),
                dma((ns, 2)), dma((ns, 2)), dma((ns, 2)), dma((ng, 2)), dma((2,)),
            ],
            compiler_params=pltpu.CompilerParams(collective_id=0, has_side_effects=True,
                                                 vmem_limit_bytes=SCOPED),
            name="stats",
        )(x_norm.T, hid_act.T, dy_out, jnp.swapaxes(dy_in, 1, 2), w_in, w_out, row_in, col_in,
          row_out.reshape(1, no), col_out.reshape(nd // LANES, LANES),
          beta_two, rel_step, clip_rms, clip_norm)
        outs = [pltpu.with_memory_space_constraint(o, pltpu.VMEM) for o in outs]
        b_out = [jax.ShapeDtypeStruct(w_in.shape, F32), jax.ShapeDtypeStruct(row_in.shape, F32),
                 jax.ShapeDtypeStruct(col_in.shape, F32), jax.ShapeDtypeStruct(w_out.shape, F32),
                 jax.ShapeDtypeStruct((1, no), F32), jax.ShapeDtypeStruct((nd // LANES, LANES), F32)]
        wi_new, ri_new, ci_new, wo_new, ro_new, co_new = pl.pallas_call(
            update_kernel,
            out_shape=b_out,
            in_specs=[vm] * len(outs),
            out_specs=[hb] * 6,
            scratch_shapes=[pltpu.VMEM((nk * ni // B_IN, B_IN, nff), F32), pltpu.VMEM((nd // CHUNK, no, CHUNK), F32),
                            dma((nk * ni // B_IN,)), dma((nd // CHUNK,)),
                            pltpu.VMEM((nk, ni), F32), pltpu.VMEM((nk, nff), F32), pltpu.VMEM((1, no), F32),
                            pltpu.VMEM((nd // LANES, LANES), F32), dma((4,))],
            compiler_params=pltpu.CompilerParams(vmem_limit_bytes=SCOPED),
            name="update",
        )(*outs)
        return (wi_new, ri_new, ci_new, wo_new, ro_new.reshape(no), co_new.reshape(nd))

    in_specs = (P(None, 'tp'), P(None, 'tp'), P(), P(), P(None, 'tp', None), P('tp', None),
                P(None, 'tp'), P(), P('tp'), P(), P(), P(), P(), P())
    out_specs = (P(None, 'tp', None), P(None, 'tp'), P(), P('tp', None), P('tp'), P())
    return jax.shard_map(local_step, mesh=mesh, in_specs=in_specs, out_specs=out_specs, check_vma=False)
```

```python
import jax
import jax.numpy as jnp
from jax import lax
from jax.experimental import pallas as pl
from jax.experimental.pallas import tpu as pltpu
from jax.sharding import PartitionSpec as P

MESH = pl.DeviceIdType.MESH
EPS_ONE = 1e-30
EPS_TWO = 1e-3
LANES = 128
F32 = jnp.float32
BF16 = jnp.bfloat16

OUT_ROW, IN_ROW, IN_STEP, STAT_ROWS = 0, 32, 64, 160
SCALAR_ROW = 24
STAGED = ((0, 32), (32, 64), (128, 32), (112, 16))
WIDE = 3
DIRECT_ROW = 96
DIRECT = ((96, 8), (104, 8))
CHUNK = 512
SUPER = 2048
HALF = 1024
SLOTS = 4
SCOPED = 30 * 1024 * 1024
PIECE = 256


def scope(name):
    pass


def lane_to_column(vec, rows):
    n = vec.shape[1]
    r = lax.broadcasted_iota(jnp.int32, (rows, n), 0)
    c = lax.broadcasted_iota(jnp.int32, (rows, n), 1)
    col = jnp.sum(jnp.where(r == c, jnp.broadcast_to(vec, (rows, n)), 0.0), axis=1, keepdims=True)
    full = jnp.broadcast_to(col, (rows, LANES))
    if rows > n:
        full = jnp.where(lax.broadcasted_iota(jnp.int32, (rows, LANES), 0) < n, full, 1.0)
    return full


def column_to_lane(col, n):
    part = col[:, :n]
    r = lax.broadcasted_iota(jnp.int32, part.shape, 0)
    c = lax.broadcasted_iota(jnp.int32, part.shape, 1)
    return jnp.sum(jnp.where(r == c, part, 0.0), axis=0, keepdims=True)


def total(x):
    return jnp.sum(jnp.sum(x, axis=0, keepdims=True), axis=1, keepdims=True)


def stats_kernel(n_dev, x_hbm, h_hbm, dyo_hbm, dyi_hbm, wi_hbm, wo_hbm, ri_hbm, ci_hbm, ro_hbm, co_hbm,
                 beta_s, rel_s, crms_s, cnorm_s,
                 di, do, wi, wo, rcol, acol, cnew, bden, kout,
                 x_v, h_v, dyo_v, ring, tail, raw, turned, ri_v, ci_v, ro_v, co_v, part, pair, tot, recv, recv_all, cden, rsum, recv2,
                 in_sem, dyo_sem, ring_sem, tail_sem, w_sem, pair_sem, chip_sem, back_sem, all_sem, two_sem):
    me = lax.axis_index('tp')
    core = lax.rem(me, 2)
    chip = me // 2
    partner = me + 1 - 2 * core
    nk, ni, nff = di.shape
    no, nd = wo.shape
    no_pad = -(-no // 8) * 8
    n_super = nff // SUPER
    tail_cols = nff - n_super * SUPER
    rows_in, rows_out = ni * n_dev, no * n_dev
    n_chip = n_dev // 2

    barrier = pltpu.get_barrier_semaphore()
    for d in range(1, n_dev):
        pl.semaphore_signal(barrier, inc=1, device_id=(lax.rem(me + d, n_dev),), device_id_type=MESH)

    scope("init")
    sequence = [(0, c) for c in range(n_super)] + [(1, c) for c in range(n_super - 1, -1, -1)]

    def half_copy(i, p):
        k, c = sequence[i]
        return pltpu.make_async_copy(dyi_hbm.at[k, pl.ds(c * SUPER + p * HALF, HALF), :],
                                     ring.at[i % SLOTS, pl.ds(p * HALF, HALF), :], ring_sem.at[i % SLOTS, p])

    def super_start(i):
        half_copy(i, 0).start()
        half_copy(i, 1).start()

    def super_wait(i):
        half_copy(i, 0).wait()
        half_copy(i, 1).wait()

    tail_cp = [pltpu.make_async_copy(dyi_hbm.at[k, pl.ds(n_super * SUPER, tail_cols), :], tail.at[k], tail_sem.at[k])
               for k in range(nk)]
    w_cp = [pltpu.make_async_copy(wi_hbm.at[k], wi.at[k], w_sem.at[k]) for k in range(nk)]
    w_cp.append(pltpu.make_async_copy(wo_hbm, wo, w_sem.at[nk]))
    small = [pltpu.make_async_copy(a, b, in_sem.at[i]) for i, (a, b) in enumerate(
        ((ro_hbm, ro_v), (ri_hbm, ri_v), (co_hbm, co_v), (ci_hbm, ci_v), (h_hbm, h_v), (x_hbm, x_v)))]
    dyo_cp = [pltpu.make_async_copy(dyo_hbm.at[:, pl.ds(c, CHUNK)], dyo_v.at[:, pl.ds(c, CHUNK)],
                                    dyo_sem.at[c // CHUNK]) for c in range(0, nd, CHUNK)]
    for cp in small[4:5] + dyo_cp[:1]:
        cp.start()
    part[...] = jnp.zeros_like(part)
    rsum[...] = jnp.zeros_like(rsum)
    dyo_cp[1].start()

    def halves(start, size, c):
        return pl.ds(pl.multiple_of(start + c * (size // 2), 8), size // 2)

    def remote(src, dst, sem, device):
        return pltpu.make_async_remote_copy(src_ref=src, dst_ref=dst, send_sem=sem.at[0], recv_sem=sem.at[1],
                                            device_id=(device,), device_id_type=MESH)

    def pair_copy(g):
        rows = halves(*STAGED[g], 1 - core)
        return remote(part.at[rows, :], pair.at[rows, :], pair_sem.at[g], partner)

    def chip_copy(g, d):
        ref = recv.at[chip, halves(*STAGED[g], core), :]
        return remote(ref, ref, chip_sem.at[g], lax.rem(me + 2 * d, n_dev))

    def back_copy(g):
        ref = tot.at[halves(*STAGED[g], core), :]
        return remote(ref, ref, back_sem.at[g], partner)

    def all_copy(g, d):
        start, size = DIRECT[g]
        ref = recv_all.at[me, pl.ds(start - DIRECT_ROW, size), :]
        return remote(ref, ref, all_sem.at[g], lax.rem(me + d, n_dev))

    def two_copy(d):
        return remote(recv2.at[me], recv2.at[me], two_sem, lax.rem(me + d, n_dev))

    def bytes_of(ref, sem):
        pltpu.make_async_copy(ref, ref, sem).wait()

    def wide_stage(g):
        rows = halves(*STAGED[g], core)
        pair_copy(g).wait_recv()
        recv[chip, rows, :] = part[rows, :] + pair[rows, :]
        for d in range(1, n_dev):
            ref = recv.at[chip, rows, :]
            remote(ref, ref, chip_sem.at[g], lax.rem(me + d, n_dev)).start()

    def wide_bytes(g, i):
        n = STAGED[g][1] // 2 * (n_dev - 1)
        bytes_of(recv.at[pl.ds(0, 5), pl.ds(0, n // 5), :], chip_sem.at[g, i])

    def chip_stage(g):
        rows = halves(*STAGED[g], core)
        pair_copy(g).wait_recv()
        recv[chip, rows, :] = part[rows, :] + pair[rows, :]
        for d in range(1, n_chip):
            chip_copy(g, d).start()

    def back_stage(g):
        start, size = STAGED[g]
        rows = halves(start, size, core)
        bytes_of(recv.at[pl.ds(0, n_chip - 1), rows, :], chip_sem.at[g, 1])
        t = recv[0, rows, :]
        for c in range(1, n_chip):
            t = t + recv[c, rows, :]
        tot[rows, :] = t
        back_copy(g).start()

    def direct_stage(g):
        start, size = DIRECT[g]
        rows = pl.ds(start - DIRECT_ROW, size)
        recv_all[me, rows, :] = part[pl.ds(start, size), :]
        for d in range(1, n_dev):
            all_copy(g, d).start()

    def square_sums(g, row0, stat0):
        m, n = g.shape
        sq = g * g
        cols = jnp.sum(sq, axis=0, keepdims=True)
        acc = rsum[pl.ds(row0, m), :]
        for b in range(0, n, LANES):
            w = min(LANES, n - b)
            if w == LANES:
                acc += sq[:, b:b + w]
                part[pl.ds(stat0 + b // LANES, 1), :] = cols[:, b:b + w]
            else:
                acc = acc + jnp.concatenate([sq[:, b:b + w], jnp.zeros((m, LANES - w), F32)], axis=1)
                part[pl.ds(stat0 + b // LANES, 1), pl.ds(0, w)] = cols[:, b:b + w]
        rsum[pl.ds(row0, m), :] = acc

    deferred = []

    def flush():
        for f in deferred:
            f()
        deferred.clear()

    def finish_in(k, col, g, store):
        if store:
            di[k, :, pl.ds(col, g.shape[1])] = g
        square_sums(g, k * ni, IN_ROW + IN_STEP * k + col // LANES)

    def finish_out(col):
        square_sums(do[:, pl.ds(col, 256)], nk * ni, OUT_ROW + col // LANES)

    def in_block(pieces, defer):
        for j, (k, col, n, ref) in enumerate(pieces):
            slot = j - len(pieces) + 2
            defer_this = defer and slot >= 0
            if j%2==1:
                turned[j % 4, :, pl.ds(0, n)] = ref[...].T
                g = jnp.dot(x_v[...], turned[j % 4, :, pl.ds(0, n)], preferred_element_type=F32)
                if defer_this:
                    di[k, :, pl.ds(col, n)] = g
                    deferred.append(lambda k=k, col=col, n=n: finish_in(k, col, di[k, :, pl.ds(col, n)], False))
                else:
                    finish_in(k, col, g, True)
            else:
                g = lax.dot_general(ref[...], x_v[...], (((1,), (1,)), ((), ())), preferred_element_type=F32)
                if defer_this:
                    raw[slot, pl.ds(0, n), :] = g
                    deferred.append(lambda k=k, col=col, n=n, slot=slot:
                                    finish_in(k, col, raw[slot, pl.ds(0, n), :].T, True))
                else:
                    finish_in(k, col, g.T, True)

    def super_pieces(i, start=0, stop=SUPER):
        k, c = sequence[i]
        return [(k, c * SUPER + p, 256, ring.at[i % SLOTS, pl.ds(p, 256), :]) for p in range(start, stop, 256)]

    def tail_pieces(k):
        return [(k, n_super * SUPER + p, min(256, tail_cols - p), tail.at[k, pl.ds(p, min(256, tail_cols - p)), :])
                for p in range(0, tail_cols, 256)]

    def out_piece(start, stop):
        for col in range(start, stop, 256):
            do[:, pl.ds(col, 256)] = jnp.dot(h_v[...], dyo_v[:, pl.ds(col, 256)], preferred_element_type=F32)
            if col + 512 >= stop:
                deferred.append(lambda col=col: finish_out(col))
            else:
                finish_out(col)

    scope("out")
    small[4].wait()
    dyo_cp[0].wait()
    for cp in dyo_cp[2:4]:
        cp.start()
    out_piece(0, CHUNK)
    dyo_cp[1].wait()
    for cp in small[:4] + dyo_cp[4:] + small[5:6]:
        cp.start()
    super_start(0)
    scope("out1")
    dyo_cp[2].wait()
    flush()
    out_piece(CHUNK, 3 * CHUNK)
    super_start(1)
    scope("out2")
    for cp in dyo_cp[3:]:
        cp.wait()
    flush()
    out_piece(3 * CHUNK, nd)
    for cp in small[:2]:
        cp.wait()
    lane = lax.broadcasted_iota(jnp.int32, (1, LANES), 1)
    row_sums = jnp.where(lane == 2, jnp.sum(ro_v[...], axis=1, keepdims=True), 0.0)
    for k in range(nk):
        row_sums += jnp.where(lane == k, jnp.sum(ri_v[pl.ds(k, 1), :], axis=1, keepdims=True), 0.0)
    part[pl.ds(SCALAR_ROW, 1), :] = row_sums
    scope("in0")
    small[5].wait()
    super_wait(0)
    super_start(2)
    tail_cp[0].start()
    flush()
    in_block(super_pieces(0), False)
    pl.semaphore_wait(barrier, n_dev - 1)
    pair_copy(0).start()
    scope("in1")
    super_wait(1)
    super_start(3)
    tail_cp[1].start()
    flush()
    in_block(super_pieces(1), False)
    chip_stage(0)
    scope("in2")
    super_wait(2)
    tail_cp[0].wait()
    super_start(4)
    flush()
    in_block(super_pieces(2) + tail_pieces(0), False)
    pair_copy(1).start()
    scope("in3")
    super_wait(3)
    tail_cp[1].wait()
    super_start(5)
    in_block(super_pieces(3) + tail_pieces(1), False)
    pair_copy(2).start()
    chip_stage(1)
    scope("in4")
    super_wait(4)
    w_cp[0].start()
    in_block(super_pieces(4), False)
    pair_copy(3).start()
    chip_stage(2)
    scope("in5")
    super_wait(5)
    for cp in w_cp[1:]:
        cp.start()
    in_block(super_pieces(5, 0, HALF), False)
    direct_stage(0)
    wide_stage(3)
    in_block(super_pieces(5, HALF, SUPER), False)
    direct_stage(1)
    back_stage(0)

    scope("forms")
    for cp in small[2:4]:
        cp.wait()
    cden[...] = jnp.ones_like(cden)
    cden[pl.ds(OUT_ROW, nd // LANES), :] = co_v[...]
    for k in range(nk):
        for q in range(nff // LANES):
            cden[pl.ds(IN_ROW + IN_STEP * k + q, 1), :] = ci_v[pl.ds(k, 1), pl.ds(q * LANES, LANES)]
        rest = nff % LANES
        if rest:
            cden[pl.ds(IN_ROW + IN_STEP * k + nff // LANES, 1), pl.ds(0, rest)] = (
                ci_v[pl.ds(k, 1), pl.ds(nff - rest, rest)])
    for k in range(nk):
        vec = ri_v[pl.ds(k, 1), :]
        for p in range(0, ni, LANES):
            n = min(LANES, ni - p)
            rcol[pl.ds(k * ni + p, n), :] = lane_to_column(vec[:, p:p + n], n)
    vec = ro_v[...]
    for p in range(0, no, LANES):
        n = min(LANES, no - p)
        rows = -(-n // 8) * 8
        rcol[pl.ds(nk * ni + p, rows), :] = lane_to_column(vec[:, p:p + n], rows)
    rsum[...] = jnp.broadcast_to(jnp.sum(rsum[...], axis=1, keepdims=True), rsum.shape)
    back_stage(1)

    def w_square_in(k):
        def body(q, acc):
            w = wi[k, :, pl.ds(pl.multiple_of(q * LANES, LANES), LANES)]
            return acc + w * w
        acc = lax.fori_loop(0, nff // LANES, body, jnp.zeros((ni, LANES), F32), unroll=4)
        rest = nff % LANES
        w = wi[k, :, pl.ds(nff - rest, rest)]
        return total(acc) + total(w * w)

    def w_square_out():
        m = no // 8 * 8
        acc = jnp.zeros((8, nd), F32)
        acc = lax.fori_loop(0, m // 8, lambda i, a: a + jnp.square(wo[pl.ds(pl.multiple_of(i * 8, 8), 8), :]), acc,
                            unroll=4)
        w = wo[pl.ds(m, no - m), :]
        return total(acc) + total(w * w)

    scope("wsq")
    w_sq = []
    for k in range(nk):
        w_cp[k].wait()
        w_sq.append(w_square_in(k))
    scope("back2")
    back_stage(2)
    scope("wsq2")
    w_cp[nk].wait()
    w_sq.append(w_square_out())

    scope("wait1")
    for g in range(WIDE):
        ref = tot.at[halves(*STAGED[g], 1 - core), :]
        bytes_of(ref, back_sem.at[g, 1])
    wide_bytes(WIDE, 1)
    rows = pl.ds(*STAGED[WIDE])
    t = recv[0, rows, :]
    for c in range(1, n_chip):
        t = t + recv[c, rows, :]
    tot[rows, :] = t
    for g in range(len(DIRECT)):
        start, size = DIRECT[g]
        rows = pl.ds(start - DIRECT_ROW, size)
        bytes_of(recv_all.at[pl.ds(0, n_dev - 1), rows, :], all_sem.at[g, 1])
    t = recv_all[0]
    for c in range(1, n_dev):
        t = t + recv_all[c]
    tot[pl.ds(DIRECT_ROW, t.shape[0]), :] = t

    scope("stats")
    beta = jnp.full((1, 1), beta_s[()], F32)
    mix = 1.0 - beta
    seg = [(IN_ROW + IN_STEP * k, IN_STEP, k * ni, ni, rows_in, nff) for k in range(nk)]
    seg.append((OUT_ROW, SCALAR_ROW, nk * ni, no_pad, rows_out, nd))
    sums = [total(tot[pl.ds(a, n), :]) for a, n, *_ in seg]
    norm_sq = sums[0] + sums[1] + sums[2]
    scale = jnp.minimum(1.0, jnp.full((1, 1), cnorm_s[()], F32) / jnp.sqrt(norm_sq))
    row_tot = tot[pl.ds(SCALAR_ROW, 1), :]
    for j, (a, n, ra, rn, m_all, n_all) in enumerate(seg):
        c2 = beta * cden[pl.ds(a, n), :] + mix * (scale * (scale * tot[pl.ds(a, n), :]) * (1.0 / m_all) + EPS_ONE)
        cnew[pl.ds(a, n), :] = c2
        bden[pl.ds(a, n), :] = scale * lax.rsqrt(c2)
        r2 = beta * rcol[pl.ds(ra, rn), :] + mix * (scale * (scale * rsum[pl.ds(ra, rn), :]) * (1.0 / n_all) + EPS_ONE)
        rcol[pl.ds(ra, rn), :] = r2
        r_all = jnp.sum(jnp.where(lane == j, row_tot, 0.0), axis=1, keepdims=True)
        level = beta * (r_all / m_all) + mix * (scale * (scale * (sums[j] / n_all)) * (1.0 / m_all) + EPS_ONE)
        acol[pl.ds(ra, rn), :] = lax.rsqrt(r2 / level)

    def u_square(ref, k, row0, m, cols, stat0, arow):
        rows = pl.ds(row0, m)

        def block(col, w, brow):
            idx = (rows, pl.ds(col, w)) if k is None else (k, rows, pl.ds(col, w))
            t = ref[idx] * jnp.broadcast_to(bden[pl.ds(brow, 1), pl.ds(0, w)], (m, w))
            return t * t

        acc = jnp.zeros((m, LANES), F32)
        for q in range(cols // LANES):
            acc = acc + block(q * LANES, LANES, stat0 + q)
        a = acol[pl.ds(arow, m), :]
        u = jnp.sum(acc * a * a, axis=0, keepdims=True)
        rest = cols % LANES
        if rest:
            a = acol[pl.ds(arow, m), pl.ds(0, rest)]
            r = jnp.sum(block(cols - rest, rest, stat0 + cols // LANES) * a * a, axis=0, keepdims=True)
            u = u + jnp.concatenate([r, jnp.zeros((1, LANES - rest), F32)], axis=1)
        return u

    scope("upass")
    u_sq = [u_square(di, k, 0, ni, nff, IN_ROW + IN_STEP * k, k * ni) for k in range(nk)]
    u_sq.append(sum(u_square(do, None, row0, m, nd, OUT_ROW, nk * ni + row0)
                    for row0, m in ((0, 144), (144, 144), (288, no - 288))))

    scope("x2")
    msg = jnp.zeros((1, LANES), F32)
    for j in range(3):
        msg = msg + jnp.where(lane == j, jnp.sum(u_sq[j], axis=1, keepdims=True), 0.0) + jnp.where(lane == 3 + j, w_sq[j], 0.0)
    recv2[me] = msg
    for d in range(1, n_dev):
        two_copy(d).start()
    pair_copy(WIDE).wait_send()
    wide_bytes(WIDE, 0)
    for g in range(WIDE):
        pair_copy(g).wait_send()
        back_copy(g).wait_send()
        bytes_of(recv.at[pl.ds(0, n_chip - 1), halves(*STAGED[g], core), :], chip_sem.at[g, 0])
    for g in range(len(DIRECT)):
        start, size = DIRECT[g]
        bytes_of(recv_all.at[pl.ds(0, n_dev - 1), pl.ds(start - DIRECT_ROW, size), :], all_sem.at[g, 0])
    bytes_of(recv2.at[pl.ds(0, n_dev - 1)], two_sem.at[1])
    scope("fin")
    all_sums = recv2[0]
    for c in range(1, n_dev):
        all_sums = all_sums + recv2[c]
    for j, (_, _, _, _, m_all, n_all) in enumerate(seg):
        u = jnp.sum(jnp.where(lane == j, all_sums, 0.0), axis=1, keepdims=True)
        w = jnp.sum(jnp.where(lane == 3 + j, all_sums, 0.0), axis=1, keepdims=True)
        u_rms = jnp.sqrt(u / (m_all * n_all))
        w_rms = jnp.sqrt(w / (m_all * n_all))
        step_size = jnp.full((1, 1), rel_s[()], F32) * jnp.maximum(EPS_TWO, w_rms)
        k = step_size / jnp.maximum(1.0, u_rms / jnp.full((1, 1), crms_s[()], F32))
        kout[pl.ds(j, 1), :] = jnp.broadcast_to(k, (1, LANES))
    bytes_of(recv2.at[pl.ds(0, n_dev - 1)], two_sem.at[0])
    scope(None)


B_IN = 32


def update_kernel(di, do, wi, wo, rcol, acol, cnew, bden, kout, wi_out, ri_hbm, ci_hbm, wo_out, ro_hbm, co_hbm,
                  buf_in, buf_out, sem_in, sem_out, ri_out, ci_out, ro_out, co_out, sem_small):
    nk, ni, nff = di.shape
    no, nd = do.shape
    steps = ni // B_IN

    def in_copy(k, i, slot):
        return pltpu.make_async_copy(buf_in.at[slot], wi_out.at[k, pl.ds(i * B_IN, B_IN), :], sem_in.at[slot])

    def widths(n):
        return [(c, min(LANES, n - c)) for c in range(0, n, LANES)]

    def step_of(w, g, b, a, kk):
        return w - kk * ((g * jnp.broadcast_to(b, g.shape)) * a)

    scope("u_in")
    pend = [None] * buf_in.shape[0]
    for k in range(nk):
        kk = jnp.broadcast_to(kout[pl.ds(k, 1), :], (B_IN, LANES))
        for i in range(steps):
            slot = (k * steps + i) % buf_in.shape[0]
            if pend[slot] is not None:
                pend[slot].wait()
            a = acol[pl.ds(k * ni + i * B_IN, B_IN), :]
            rows = pl.ds(i * B_IN, B_IN)
            for q, (c, n) in enumerate(widths(nff)):
                cc = pl.ds(c, n)
                b = bden[pl.ds(IN_ROW + IN_STEP * k + q, 1), pl.ds(0, n)]
                buf_in[slot, :, cc] = step_of(wi[k, rows, cc], di[k, rows, cc], b, a[:, :n], kk[:, :n])
            cp = in_copy(k, i, slot)
            cp.start()
            pend[slot] = cp
    scope("u_small")
    co_out[...] = cnew[pl.ds(OUT_ROW, nd // LANES), :]
    for k in range(nk):
        for c, n in widths(nff):
            ci_out[pl.ds(k, 1), pl.ds(c, n)] = cnew[pl.ds(IN_ROW + IN_STEP * k + c // LANES, 1), pl.ds(0, n)]
        for c, n in widths(ni):
            ri_out[pl.ds(k, 1), pl.ds(c, n)] = column_to_lane(rcol[pl.ds(k * ni + c, n), :], n)
    for c, n in widths(no):
        ro_out[:, pl.ds(c, n)] = column_to_lane(rcol[pl.ds(nk * ni + c, -(-n // 8) * 8), :], n)
    small = [pltpu.make_async_copy(v, h, sem_small.at[i]) for i, (v, h) in enumerate(
        ((ri_out, ri_hbm), (ci_out, ci_hbm), (ro_out, ro_hbm), (co_out, co_hbm)))]
    for cp in small:
        cp.start()
    scope("u_out")
    pend_out = [None] * buf_out.shape[0]
    for i in range(nd // CHUNK):
        slot = i % buf_out.shape[0]
        if pend_out[slot] is not None:
            pend_out[slot].wait()
        kk = jnp.broadcast_to(kout[pl.ds(nk, 1), :], (40, LANES))
        bs = [bden[pl.ds(OUT_ROW + i * (CHUNK // LANES) + q, 1), :] for q in range(CHUNK // LANES)]

        def rows_of(o, n, i=i, slot=slot, kk=kk, bs=bs):
            r = pl.ds(o, n)
            a = acol[pl.ds(nk * ni + o, n), :]
            for q, b in enumerate(bs):
                cc = pl.ds(i * CHUNK + q * LANES, LANES)
                buf_out[slot, r, pl.ds(q * LANES, LANES)] = step_of(wo[r, cc], do[r, cc], b, a, kk[:n])

        for o in range(0, no, 40):
            rows_of(o, min(40, no - o))
        cp = pltpu.make_async_copy(buf_out.at[slot], wo_out.at[:, pl.ds(i * CHUNK, CHUNK)], sem_out.at[slot])
        cp.start()
        pend_out[slot] = cp
    scope("u_wait")
    for cp in pend + pend_out + small:
        if cp is not None:
            cp.wait()
    scope(None)


def solution(mesh):
    n_dev = mesh.shape['tp']

    def local_step(x_norm, hid_act, dy_in, dy_out, w_in, w_out, row_in, col_in, row_out, col_out,
                   beta_two, rel_step, clip_rms, clip_norm):
        t, ni = x_norm.shape
        no = hid_act.shape[1]
        nk, _, nff = dy_in.shape
        nd = dy_out.shape[1]
        no_pad = -(-no // 8) * 8
        tail_cols = nff - nff // SUPER * SUPER
        vm = pl.BlockSpec(memory_space=pltpu.VMEM)
        hb = pl.BlockSpec(memory_space=pltpu.HBM)
        sm = pl.BlockSpec(memory_space=pltpu.SMEM)
        dma = pltpu.SemaphoreType.DMA
        n_rows = nk * ni + no_pad
        a_out = [pltpu.VMEM((nk, ni, nff), F32), pltpu.VMEM((no, nd), F32),
                 pltpu.VMEM((nk, ni, nff), F32), pltpu.VMEM((no, nd), F32),
                 pltpu.VMEM((n_rows, LANES), F32), pltpu.VMEM((n_rows, LANES), F32),
                 pltpu.VMEM((STAT_ROWS, LANES), F32), pltpu.VMEM((STAT_ROWS, LANES), F32),
                 pltpu.VMEM((8, LANES), F32)]
        ns, ng = len(STAGED), len(DIRECT)
        stat = pltpu.VMEM((STAT_ROWS, LANES), F32)
        outs = pl.pallas_call(
            lambda *refs: stats_kernel(n_dev, *refs),
            out_shape=a_out,
            in_specs=[hb] * 10 + [sm] * 4,
            out_specs=[vm] * len(a_out),
            scratch_shapes=[
                pltpu.VMEM((ni, t), BF16), pltpu.VMEM((no, t), BF16), pltpu.VMEM((t, nd), BF16),
                pltpu.VMEM((SLOTS, SUPER, t), BF16), pltpu.VMEM((nk, tail_cols, t), BF16), pltpu.VMEM((2, 256, ni), F32), pltpu.VMEM((4, t, 256), BF16),
                pltpu.VMEM((nk, ni), F32), pltpu.VMEM((nk, nff), F32), pltpu.VMEM((1, no), F32),
                pltpu.VMEM((nd // LANES, LANES), F32),
                stat, stat, stat, pltpu.VMEM((n_dev // 2, STAT_ROWS, LANES), F32),
                pltpu.VMEM((n_dev, sum(n for _, n in DIRECT), LANES), F32), stat,
                pltpu.VMEM((n_rows, LANES), F32), pltpu.VMEM((n_dev, 1, LANES), F32),
                dma((6,)), dma((nd // CHUNK,)), dma((SLOTS, 2)), dma((nk,)), dma((nk + 1,)),
                dma((ns, 2)), dma((ns, 2)), dma((ns, 2)), dma((ng, 2)), dma((2,)),
            ],
            compiler_params=pltpu.CompilerParams(collective_id=0, has_side_effects=True,
                                                 vmem_limit_bytes=SCOPED),
            name="stats",
        )(x_norm.T, hid_act.T, dy_out, jnp.swapaxes(dy_in, 1, 2), w_in, w_out, row_in, col_in,
          row_out.reshape(1, no), col_out.reshape(nd // LANES, LANES),
          beta_two, rel_step, clip_rms, clip_norm)
        outs = [pltpu.with_memory_space_constraint(o, pltpu.VMEM) for o in outs]
        b_out = [jax.ShapeDtypeStruct(w_in.shape, F32), jax.ShapeDtypeStruct(row_in.shape, F32),
                 jax.ShapeDtypeStruct(col_in.shape, F32), jax.ShapeDtypeStruct(w_out.shape, F32),
                 jax.ShapeDtypeStruct((1, no), F32), jax.ShapeDtypeStruct((nd // LANES, LANES), F32)]
        wi_new, ri_new, ci_new, wo_new, ro_new, co_new = pl.pallas_call(
            update_kernel,
            out_shape=b_out,
            in_specs=[vm] * len(outs),
            out_specs=[hb] * 6,
            scratch_shapes=[pltpu.VMEM((nk * ni // B_IN, B_IN, nff), F32), pltpu.VMEM((nd // CHUNK, no, CHUNK), F32),
                            dma((nk * ni // B_IN,)), dma((nd // CHUNK,)),
                            pltpu.VMEM((nk, ni), F32), pltpu.VMEM((nk, nff), F32), pltpu.VMEM((1, no), F32),
                            pltpu.VMEM((nd // LANES, LANES), F32), dma((4,))],
            compiler_params=pltpu.CompilerParams(vmem_limit_bytes=SCOPED),
            name="update",
        )(*outs)
        return (wi_new, ri_new, ci_new, wo_new, ro_new.reshape(no), co_new.reshape(nd))

    in_specs = (P(None, 'tp'), P(None, 'tp'), P(), P(), P(None, 'tp', None), P('tp', None),
                P(None, 'tp'), P(), P('tp'), P(), P(), P(), P(), P())
    out_specs = (P(None, 'tp', None), P(None, 'tp'), P(), P('tp', None), P('tp'), P())
    return jax.shard_map(local_step, mesh=mesh, in_specs=in_specs, out_specs=out_specs, check_vma=False)
```

```python
import jax
import jax.numpy as jnp
from jax import lax
from jax.experimental import pallas as pl
from jax.experimental.pallas import tpu as pltpu
from jax.sharding import PartitionSpec as P

MESH = pl.DeviceIdType.MESH
EPS_ONE = 1e-30
EPS_TWO = 1e-3
LANES = 128
F32 = jnp.float32
BF16 = jnp.bfloat16

OUT_ROW, IN_ROW, IN_STEP, STAT_ROWS = 0, 32, 64, 160
SCALAR_ROW = 24
STAGED = ((0, 32), (32, 64), (128, 32), (112, 16))
WIDE = 3
DIRECT_ROW = 96
DIRECT = ((96, 8), (104, 8))
CHUNK = 512
SUPER = 2048
HALF = 1024
SLOTS = 4
SCOPED = 30 * 1024 * 1024
PIECE = 256


def scope(name):
    pass


def lane_to_column(vec, rows):
    n = vec.shape[1]
    r = lax.broadcasted_iota(jnp.int32, (rows, n), 0)
    c = lax.broadcasted_iota(jnp.int32, (rows, n), 1)
    col = jnp.sum(jnp.where(r == c, jnp.broadcast_to(vec, (rows, n)), 0.0), axis=1, keepdims=True)
    full = jnp.broadcast_to(col, (rows, LANES))
    if rows > n:
        full = jnp.where(lax.broadcasted_iota(jnp.int32, (rows, LANES), 0) < n, full, 1.0)
    return full


def column_to_lane(col, n):
    part = col[:, :n]
    r = lax.broadcasted_iota(jnp.int32, part.shape, 0)
    c = lax.broadcasted_iota(jnp.int32, part.shape, 1)
    return jnp.sum(jnp.where(r == c, part, 0.0), axis=0, keepdims=True)


def total(x):
    return jnp.sum(jnp.sum(x, axis=0, keepdims=True), axis=1, keepdims=True)


def stats_kernel(n_dev, x_hbm, h_hbm, dyo_hbm, dyi_hbm, wi_hbm, wo_hbm, ri_hbm, ci_hbm, ro_hbm, co_hbm,
                 beta_s, rel_s, crms_s, cnorm_s,
                 di, do, wi, wo, rcol, acol, cnew, bden, kout,
                 x_v, h_v, dyo_v, ring, tail, raw, turned, ri_v, ci_v, ro_v, co_v, part, pair, tot, recv, recv_all, cden, rsum, recv2,
                 in_sem, dyo_sem, ring_sem, tail_sem, w_sem, pair_sem, chip_sem, back_sem, all_sem, two_sem):
    me = lax.axis_index('tp')
    core = lax.rem(me, 2)
    chip = me // 2
    partner = me + 1 - 2 * core
    nk, ni, nff = di.shape
    no, nd = wo.shape
    no_pad = -(-no // 8) * 8
    n_super = nff // SUPER
    tail_cols = nff - n_super * SUPER
    rows_in, rows_out = ni * n_dev, no * n_dev
    n_chip = n_dev // 2

    barrier = pltpu.get_barrier_semaphore()
    for d in range(1, n_dev):
        pl.semaphore_signal(barrier, inc=1, device_id=(lax.rem(me + d, n_dev),), device_id_type=MESH)

    scope("init")
    sequence = [(0, c) for c in range(n_super)] + [(1, c) for c in range(n_super - 1, -1, -1)]

    def half_copy(i, p):
        k, c = sequence[i]
        return pltpu.make_async_copy(dyi_hbm.at[k, pl.ds(c * SUPER + p * HALF, HALF), :],
                                     ring.at[i % SLOTS, pl.ds(p * HALF, HALF), :], ring_sem.at[i % SLOTS, p])

    def super_start(i):
        half_copy(i, 0).start()
        half_copy(i, 1).start()

    def super_wait(i):
        half_copy(i, 0).wait()
        half_copy(i, 1).wait()

    tail_cp = [pltpu.make_async_copy(dyi_hbm.at[k, pl.ds(n_super * SUPER, tail_cols), :], tail.at[k], tail_sem.at[k])
               for k in range(nk)]
    w_cp = [pltpu.make_async_copy(wi_hbm.at[k], wi.at[k], w_sem.at[k]) for k in range(nk)]
    w_cp.append(pltpu.make_async_copy(wo_hbm, wo, w_sem.at[nk]))
    small = [pltpu.make_async_copy(a, b, in_sem.at[i]) for i, (a, b) in enumerate(
        ((ro_hbm, ro_v), (ri_hbm, ri_v), (co_hbm, co_v), (ci_hbm, ci_v), (h_hbm, h_v), (x_hbm, x_v)))]
    dyo_cp = [pltpu.make_async_copy(dyo_hbm.at[:, pl.ds(c, CHUNK)], dyo_v.at[:, pl.ds(c, CHUNK)],
                                    dyo_sem.at[c // CHUNK]) for c in range(0, nd, CHUNK)]
    for cp in small[4:5] + dyo_cp[:1]:
        cp.start()
    part[...] = jnp.zeros_like(part)
    rsum[...] = jnp.zeros_like(rsum)
    for cp in dyo_cp[1:3]:
        cp.start()

    def halves(start, size, c):
        return pl.ds(pl.multiple_of(start + c * (size // 2), 8), size // 2)

    def remote(src, dst, sem, device):
        return pltpu.make_async_remote_copy(src_ref=src, dst_ref=dst, send_sem=sem.at[0], recv_sem=sem.at[1],
                                            device_id=(device,), device_id_type=MESH)

    def pair_copy(g):
        rows = halves(*STAGED[g], 1 - core)
        return remote(part.at[rows, :], pair.at[rows, :], pair_sem.at[g], partner)

    def chip_copy(g, d):
        ref = recv.at[chip, halves(*STAGED[g], core), :]
        return remote(ref, ref, chip_sem.at[g], lax.rem(me + 2 * d, n_dev))

    def back_copy(g):
        ref = tot.at[halves(*STAGED[g], core), :]
        return remote(ref, ref, back_sem.at[g], partner)

    def all_copy(g, d):
        start, size = DIRECT[g]
        ref = recv_all.at[me, pl.ds(start - DIRECT_ROW, size), :]
        return remote(ref, ref, all_sem.at[g], lax.rem(me + d, n_dev))

    def two_copy(d):
        return remote(recv2.at[me], recv2.at[me], two_sem, lax.rem(me + d, n_dev))

    def bytes_of(ref, sem):
        pltpu.make_async_copy(ref, ref, sem).wait()

    def wide_stage(g):
        rows = halves(*STAGED[g], core)
        pair_copy(g).wait_recv()
        recv[chip, rows, :] = part[rows, :] + pair[rows, :]
        for d in range(1, n_dev):
            ref = recv.at[chip, rows, :]
            remote(ref, ref, chip_sem.at[g], lax.rem(me + d, n_dev)).start()

    def wide_bytes(g, i):
        n = STAGED[g][1] // 2 * (n_dev - 1)
        bytes_of(recv.at[pl.ds(0, 5), pl.ds(0, n // 5), :], chip_sem.at[g, i])

    def chip_stage(g):
        rows = halves(*STAGED[g], core)
        pair_copy(g).wait_recv()
        recv[chip, rows, :] = part[rows, :] + pair[rows, :]
        for d in range(1, n_chip):
            chip_copy(g, d).start()

    def back_stage(g):
        start, size = STAGED[g]
        rows = halves(start, size, core)
        bytes_of(recv.at[pl.ds(0, n_chip - 1), rows, :], chip_sem.at[g, 1])
        t = recv[0, rows, :]
        for c in range(1, n_chip):
            t = t + recv[c, rows, :]
        tot[rows, :] = t
        back_copy(g).start()

    def direct_stage(g):
        start, size = DIRECT[g]
        rows = pl.ds(start - DIRECT_ROW, size)
        recv_all[me, rows, :] = part[pl.ds(start, size), :]
        for d in range(1, n_dev):
            all_copy(g, d).start()

    def square_sums(g, row0, stat0):
        m, n = g.shape
        sq = g * g
        cols = jnp.sum(sq, axis=0, keepdims=True)
        acc = rsum[pl.ds(row0, m), :]
        for b in range(0, n, LANES):
            w = min(LANES, n - b)
            if w == LANES:
                acc += sq[:, b:b + w]
                part[pl.ds(stat0 + b // LANES, 1), :] = cols[:, b:b + w]
            else:
                acc = acc + jnp.concatenate([sq[:, b:b + w], jnp.zeros((m, LANES - w), F32)], axis=1)
                part[pl.ds(stat0 + b // LANES, 1), pl.ds(0, w)] = cols[:, b:b + w]
        rsum[pl.ds(row0, m), :] = acc

    deferred = []

    def flush():
        for f in deferred:
            f()
        deferred.clear()

    def finish_in(k, col, g, store):
        if store:
            di[k, :, pl.ds(col, g.shape[1])] = g
        square_sums(g, k * ni, IN_ROW + IN_STEP * k + col // LANES)

    def finish_out(col):
        square_sums(do[:, pl.ds(col, 256)], nk * ni, OUT_ROW + col // LANES)

    def in_block(pieces, defer):
        for j, (k, col, n, ref) in enumerate(pieces):
            slot = j - len(pieces) + 2
            defer_this = defer and slot >= 0
            if j%2==1:
                turned[j % 4, :, pl.ds(0, n)] = ref[...].T
                g = jnp.dot(x_v[...], turned[j % 4, :, pl.ds(0, n)], preferred_element_type=F32)
                if defer_this:
                    di[k, :, pl.ds(col, n)] = g
                    deferred.append(lambda k=k, col=col, n=n: finish_in(k, col, di[k, :, pl.ds(col, n)], False))
                else:
                    finish_in(k, col, g, True)
            else:
                g = lax.dot_general(ref[...], x_v[...], (((1,), (1,)), ((), ())), preferred_element_type=F32)
                if defer_this:
                    raw[slot, pl.ds(0, n), :] = g
                    deferred.append(lambda k=k, col=col, n=n, slot=slot:
                                    finish_in(k, col, raw[slot, pl.ds(0, n), :].T, True))
                else:
                    finish_in(k, col, g.T, True)

    def super_pieces(i, start=0, stop=SUPER):
        k, c = sequence[i]
        return [(k, c * SUPER + p, 256, ring.at[i % SLOTS, pl.ds(p, 256), :]) for p in range(start, stop, 256)]

    def tail_pieces(k):
        return [(k, n_super * SUPER + p, min(256, tail_cols - p), tail.at[k, pl.ds(p, min(256, tail_cols - p)), :])
                for p in range(0, tail_cols, 256)]

    def out_piece(start, stop):
        for col in range(start, stop, 256):
            do[:, pl.ds(col, 256)] = jnp.dot(h_v[...], dyo_v[:, pl.ds(col, 256)], preferred_element_type=F32)
            if col + 512 >= stop:
                deferred.append(lambda col=col: finish_out(col))
            else:
                finish_out(col)

    scope("out")
    small[4].wait()
    dyo_cp[0].wait()
    for cp in dyo_cp[3:] + small[5:6]:
        cp.start()
    half_copy(0, 0).start()
    out_piece(0, CHUNK)
    dyo_cp[1].wait()
    for cp in small[:4]:
        cp.start()
    half_copy(0, 1).start()
    scope("out1")
    dyo_cp[2].wait()
    flush()
    out_piece(CHUNK, 3 * CHUNK)
    super_start(1)
    scope("out2")
    for cp in dyo_cp[3:]:
        cp.wait()
    flush()
    out_piece(3 * CHUNK, nd)
    for cp in small[:2]:
        cp.wait()
    lane = lax.broadcasted_iota(jnp.int32, (1, LANES), 1)
    row_sums = jnp.where(lane == 2, jnp.sum(ro_v[...], axis=1, keepdims=True), 0.0)
    for k in range(nk):
        row_sums += jnp.where(lane == k, jnp.sum(ri_v[pl.ds(k, 1), :], axis=1, keepdims=True), 0.0)
    part[pl.ds(SCALAR_ROW, 1), :] = row_sums
    scope("in0")
    small[5].wait()
    super_wait(0)
    super_start(2)
    tail_cp[0].start()
    flush()
    in_block(super_pieces(0), False)
    pl.semaphore_wait(barrier, n_dev - 1)
    pair_copy(0).start()
    scope("in1")
    super_wait(1)
    super_start(3)
    tail_cp[1].start()
    flush()
    in_block(super_pieces(1), False)
    chip_stage(0)
    scope("in2")
    super_wait(2)
    tail_cp[0].wait()
    super_start(4)
    flush()
    in_block(super_pieces(2) + tail_pieces(0), False)
    pair_copy(1).start()
    scope("in3")
    super_wait(3)
    tail_cp[1].wait()
    super_start(5)
    in_block(super_pieces(3) + tail_pieces(1), False)
    pair_copy(2).start()
    chip_stage(1)
    scope("in4")
    super_wait(4)
    w_cp[0].start()
    in_block(super_pieces(4), False)
    pair_copy(3).start()
    chip_stage(2)
    scope("in5")
    super_wait(5)
    for cp in w_cp[1:]:
        cp.start()
    in_block(super_pieces(5, 0, HALF), False)
    direct_stage(0)
    wide_stage(3)
    in_block(super_pieces(5, HALF, SUPER), False)
    direct_stage(1)
    back_stage(0)

    scope("forms")
    for cp in small[2:4]:
        cp.wait()
    cden[...] = jnp.ones_like(cden)
    cden[pl.ds(OUT_ROW, nd // LANES), :] = co_v[...]
    for k in range(nk):
        for q in range(nff // LANES):
            cden[pl.ds(IN_ROW + IN_STEP * k + q, 1), :] = ci_v[pl.ds(k, 1), pl.ds(q * LANES, LANES)]
        rest = nff % LANES
        if rest:
            cden[pl.ds(IN_ROW + IN_STEP * k + nff // LANES, 1), pl.ds(0, rest)] = (
                ci_v[pl.ds(k, 1), pl.ds(nff - rest, rest)])
    for k in range(nk):
        vec = ri_v[pl.ds(k, 1), :]
        for p in range(0, ni, LANES):
            n = min(LANES, ni - p)
            rcol[pl.ds(k * ni + p, n), :] = lane_to_column(vec[:, p:p + n], n)
    vec = ro_v[...]
    for p in range(0, no, LANES):
        n = min(LANES, no - p)
        rows = -(-n // 8) * 8
        rcol[pl.ds(nk * ni + p, rows), :] = lane_to_column(vec[:, p:p + n], rows)
    rsum[...] = jnp.broadcast_to(jnp.sum(rsum[...], axis=1, keepdims=True), rsum.shape)
    back_stage(1)

    def w_square_in(k):
        def body(q, acc):
            w = wi[k, :, pl.ds(pl.multiple_of(q * LANES, LANES), LANES)]
            return acc + w * w
        acc = lax.fori_loop(0, nff // LANES, body, jnp.zeros((ni, LANES), F32), unroll=4)
        rest = nff % LANES
        w = wi[k, :, pl.ds(nff - rest, rest)]
        return total(acc) + total(w * w)

    def w_square_out():
        m = no // 8 * 8
        acc = jnp.zeros((8, nd), F32)
        acc = lax.fori_loop(0, m // 8, lambda i, a: a + jnp.square(wo[pl.ds(pl.multiple_of(i * 8, 8), 8), :]), acc,
                            unroll=4)
        w = wo[pl.ds(m, no - m), :]
        return total(acc) + total(w * w)

    scope("wsq")
    w_sq = []
    for k in range(nk):
        w_cp[k].wait()
        w_sq.append(w_square_in(k))
    scope("back2")
    back_stage(2)
    scope("wsq2")
    w_cp[nk].wait()
    w_sq.append(w_square_out())

    scope("wait1")
    for g in range(WIDE):
        ref = tot.at[halves(*STAGED[g], 1 - core), :]
        bytes_of(ref, back_sem.at[g, 1])
    wide_bytes(WIDE, 1)
    rows = pl.ds(*STAGED[WIDE])
    t = recv[0, rows, :]
    for c in range(1, n_chip):
        t = t + recv[c, rows, :]
    tot[rows, :] = t
    for g in range(len(DIRECT)):
        start, size = DIRECT[g]
        rows = pl.ds(start - DIRECT_ROW, size)
        bytes_of(recv_all.at[pl.ds(0, n_dev - 1), rows, :], all_sem.at[g, 1])
    t = recv_all[0]
    for c in range(1, n_dev):
        t = t + recv_all[c]
    tot[pl.ds(DIRECT_ROW, t.shape[0]), :] = t

    scope("stats")
    beta = jnp.full((1, 1), beta_s[()], F32)
    mix = 1.0 - beta
    seg = [(IN_ROW + IN_STEP * k, IN_STEP, k * ni, ni, rows_in, nff) for k in range(nk)]
    seg.append((OUT_ROW, SCALAR_ROW, nk * ni, no_pad, rows_out, nd))
    sums = [total(tot[pl.ds(a, n), :]) for a, n, *_ in seg]
    norm_sq = sums[0] + sums[1] + sums[2]
    scale = jnp.minimum(1.0, jnp.full((1, 1), cnorm_s[()], F32) / jnp.sqrt(norm_sq))
    row_tot = tot[pl.ds(SCALAR_ROW, 1), :]
    for j, (a, n, ra, rn, m_all, n_all) in enumerate(seg):
        c2 = beta * cden[pl.ds(a, n), :] + mix * (scale * (scale * tot[pl.ds(a, n), :]) * (1.0 / m_all) + EPS_ONE)
        cnew[pl.ds(a, n), :] = c2
        bden[pl.ds(a, n), :] = scale * lax.rsqrt(c2)
        r2 = beta * rcol[pl.ds(ra, rn), :] + mix * (scale * (scale * rsum[pl.ds(ra, rn), :]) * (1.0 / n_all) + EPS_ONE)
        rcol[pl.ds(ra, rn), :] = r2
        r_all = jnp.sum(jnp.where(lane == j, row_tot, 0.0), axis=1, keepdims=True)
        level = beta * (r_all / m_all) + mix * (scale * (scale * (sums[j] / n_all)) * (1.0 / m_all) + EPS_ONE)
        acol[pl.ds(ra, rn), :] = lax.rsqrt(r2 / level)

    def u_square(ref, k, row0, m, cols, stat0, arow):
        rows = pl.ds(row0, m)

        def block(col, w, brow):
            idx = (rows, pl.ds(col, w)) if k is None else (k, rows, pl.ds(col, w))
            t = ref[idx] * jnp.broadcast_to(bden[pl.ds(brow, 1), pl.ds(0, w)], (m, w))
            return t * t

        acc = jnp.zeros((m, LANES), F32)
        for q in range(cols // LANES):
            acc = acc + block(q * LANES, LANES, stat0 + q)
        a = acol[pl.ds(arow, m), :]
        u = jnp.sum(acc * a * a, axis=0, keepdims=True)
        rest = cols % LANES
        if rest:
            a = acol[pl.ds(arow, m), pl.ds(0, rest)]
            r = jnp.sum(block(cols - rest, rest, stat0 + cols // LANES) * a * a, axis=0, keepdims=True)
            u = u + jnp.concatenate([r, jnp.zeros((1, LANES - rest), F32)], axis=1)
        return u

    scope("upass")
    u_sq = [u_square(di, k, 0, ni, nff, IN_ROW + IN_STEP * k, k * ni) for k in range(nk)]
    u_sq.append(sum(u_square(do, None, row0, m, nd, OUT_ROW, nk * ni + row0)
                    for row0, m in ((0, 144), (144, 144), (288, no - 288))))

    scope("x2")
    msg = jnp.zeros((1, LANES), F32)
    for j in range(3):
        msg = msg + jnp.where(lane == j, jnp.sum(u_sq[j], axis=1, keepdims=True), 0.0) + jnp.where(lane == 3 + j, w_sq[j], 0.0)
    recv2[me] = msg
    for d in range(1, n_dev):
        two_copy(d).start()
    pair_copy(WIDE).wait_send()
    wide_bytes(WIDE, 0)
    for g in range(WIDE):
        pair_copy(g).wait_send()
        back_copy(g).wait_send()
        bytes_of(recv.at[pl.ds(0, n_chip - 1), halves(*STAGED[g], core), :], chip_sem.at[g, 0])
    for g in range(len(DIRECT)):
        start, size = DIRECT[g]
        bytes_of(recv_all.at[pl.ds(0, n_dev - 1), pl.ds(start - DIRECT_ROW, size), :], all_sem.at[g, 0])
    bytes_of(recv2.at[pl.ds(0, n_dev - 1)], two_sem.at[1])
    scope("fin")
    all_sums = recv2[0]
    for c in range(1, n_dev):
        all_sums = all_sums + recv2[c]
    for j, (_, _, _, _, m_all, n_all) in enumerate(seg):
        u = jnp.sum(jnp.where(lane == j, all_sums, 0.0), axis=1, keepdims=True)
        w = jnp.sum(jnp.where(lane == 3 + j, all_sums, 0.0), axis=1, keepdims=True)
        u_rms = jnp.sqrt(u / (m_all * n_all))
        w_rms = jnp.sqrt(w / (m_all * n_all))
        step_size = jnp.full((1, 1), rel_s[()], F32) * jnp.maximum(EPS_TWO, w_rms)
        k = step_size / jnp.maximum(1.0, u_rms / jnp.full((1, 1), crms_s[()], F32))
        kout[pl.ds(j, 1), :] = jnp.broadcast_to(k, (1, LANES))
    bytes_of(recv2.at[pl.ds(0, n_dev - 1)], two_sem.at[0])
    scope(None)


B_IN = 32


def update_kernel(di, do, wi, wo, rcol, acol, cnew, bden, kout, wi_out, ri_hbm, ci_hbm, wo_out, ro_hbm, co_hbm,
                  buf_in, buf_out, sem_in, sem_out, ri_out, ci_out, ro_out, co_out, sem_small):
    nk, ni, nff = di.shape
    no, nd = do.shape
    steps = ni // B_IN

    def in_copy(k, i, slot):
        return pltpu.make_async_copy(buf_in.at[slot], wi_out.at[k, pl.ds(i * B_IN, B_IN), :], sem_in.at[slot])

    def widths(n):
        return [(c, min(LANES, n - c)) for c in range(0, n, LANES)]

    def step_of(w, g, b, a, kk):
        return w - kk * ((g * jnp.broadcast_to(b, g.shape)) * a)

    scope("u_in")
    pend = [None] * buf_in.shape[0]
    for k in range(nk):
        kk = jnp.broadcast_to(kout[pl.ds(k, 1), :], (B_IN, LANES))
        for i in range(steps):
            slot = (k * steps + i) % buf_in.shape[0]
            if pend[slot] is not None:
                pend[slot].wait()
            a = acol[pl.ds(k * ni + i * B_IN, B_IN), :]
            rows = pl.ds(i * B_IN, B_IN)
            for q, (c, n) in enumerate(widths(nff)):
                cc = pl.ds(c, n)
                b = bden[pl.ds(IN_ROW + IN_STEP * k + q, 1), pl.ds(0, n)]
                buf_in[slot, :, cc] = step_of(wi[k, rows, cc], di[k, rows, cc], b, a[:, :n], kk[:, :n])
            cp = in_copy(k, i, slot)
            cp.start()
            pend[slot] = cp
    scope("u_small")
    co_out[...] = cnew[pl.ds(OUT_ROW, nd // LANES), :]
    for k in range(nk):
        for c, n in widths(nff):
            ci_out[pl.ds(k, 1), pl.ds(c, n)] = cnew[pl.ds(IN_ROW + IN_STEP * k + c // LANES, 1), pl.ds(0, n)]
        for c, n in widths(ni):
            ri_out[pl.ds(k, 1), pl.ds(c, n)] = column_to_lane(rcol[pl.ds(k * ni + c, n), :], n)
    for c, n in widths(no):
        ro_out[:, pl.ds(c, n)] = column_to_lane(rcol[pl.ds(nk * ni + c, -(-n // 8) * 8), :], n)
    small = [pltpu.make_async_copy(v, h, sem_small.at[i]) for i, (v, h) in enumerate(
        ((ri_out, ri_hbm), (ci_out, ci_hbm), (ro_out, ro_hbm), (co_out, co_hbm)))]
    for cp in small:
        cp.start()
    scope("u_out")
    pend_out = [None] * buf_out.shape[0]
    for i in range(nd // CHUNK):
        slot = i % buf_out.shape[0]
        if pend_out[slot] is not None:
            pend_out[slot].wait()
        kk = jnp.broadcast_to(kout[pl.ds(nk, 1), :], (40, LANES))
        bs = [bden[pl.ds(OUT_ROW + i * (CHUNK // LANES) + q, 1), :] for q in range(CHUNK // LANES)]

        def rows_of(o, n, i=i, slot=slot, kk=kk, bs=bs):
            r = pl.ds(o, n)
            a = acol[pl.ds(nk * ni + o, n), :]
            for q, b in enumerate(bs):
                cc = pl.ds(i * CHUNK + q * LANES, LANES)
                buf_out[slot, r, pl.ds(q * LANES, LANES)] = step_of(wo[r, cc], do[r, cc], b, a, kk[:n])

        for o in range(0, no, 40):
            rows_of(o, min(40, no - o))
        cp = pltpu.make_async_copy(buf_out.at[slot], wo_out.at[:, pl.ds(i * CHUNK, CHUNK)], sem_out.at[slot])
        cp.start()
        pend_out[slot] = cp
    scope("u_wait")
    for cp in pend + pend_out + small:
        if cp is not None:
            cp.wait()
    scope(None)


def solution(mesh):
    n_dev = mesh.shape['tp']

    def local_step(x_norm, hid_act, dy_in, dy_out, w_in, w_out, row_in, col_in, row_out, col_out,
                   beta_two, rel_step, clip_rms, clip_norm):
        t, ni = x_norm.shape
        no = hid_act.shape[1]
        nk, _, nff = dy_in.shape
        nd = dy_out.shape[1]
        no_pad = -(-no // 8) * 8
        tail_cols = nff - nff // SUPER * SUPER
        vm = pl.BlockSpec(memory_space=pltpu.VMEM)
        hb = pl.BlockSpec(memory_space=pltpu.HBM)
        sm = pl.BlockSpec(memory_space=pltpu.SMEM)
        dma = pltpu.SemaphoreType.DMA
        n_rows = nk * ni + no_pad
        a_out = [pltpu.VMEM((nk, ni, nff), F32), pltpu.VMEM((no, nd), F32),
                 pltpu.VMEM((nk, ni, nff), F32), pltpu.VMEM((no, nd), F32),
                 pltpu.VMEM((n_rows, LANES), F32), pltpu.VMEM((n_rows, LANES), F32),
                 pltpu.VMEM((STAT_ROWS, LANES), F32), pltpu.VMEM((STAT_ROWS, LANES), F32),
                 pltpu.VMEM((8, LANES), F32)]
        ns, ng = len(STAGED), len(DIRECT)
        stat = pltpu.VMEM((STAT_ROWS, LANES), F32)
        outs = pl.pallas_call(
            lambda *refs: stats_kernel(n_dev, *refs),
            out_shape=a_out,
            in_specs=[hb] * 10 + [sm] * 4,
            out_specs=[vm] * len(a_out),
            scratch_shapes=[
                pltpu.VMEM((ni, t), BF16), pltpu.VMEM((no, t), BF16), pltpu.VMEM((t, nd), BF16),
                pltpu.VMEM((SLOTS, SUPER, t), BF16), pltpu.VMEM((nk, tail_cols, t), BF16), pltpu.VMEM((2, 256, ni), F32), pltpu.VMEM((4, t, 256), BF16),
                pltpu.VMEM((nk, ni), F32), pltpu.VMEM((nk, nff), F32), pltpu.VMEM((1, no), F32),
                pltpu.VMEM((nd // LANES, LANES), F32),
                stat, stat, stat, pltpu.VMEM((n_dev // 2, STAT_ROWS, LANES), F32),
                pltpu.VMEM((n_dev, sum(n for _, n in DIRECT), LANES), F32), stat,
                pltpu.VMEM((n_rows, LANES), F32), pltpu.VMEM((n_dev, 1, LANES), F32),
                dma((6,)), dma((nd // CHUNK,)), dma((SLOTS, 2)), dma((nk,)), dma((nk + 1,)),
                dma((ns, 2)), dma((ns, 2)), dma((ns, 2)), dma((ng, 2)), dma((2,)),
            ],
            compiler_params=pltpu.CompilerParams(collective_id=0, has_side_effects=True,
                                                 vmem_limit_bytes=SCOPED),
            name="stats",
        )(x_norm.T, hid_act.T, dy_out, jnp.swapaxes(dy_in, 1, 2), w_in, w_out, row_in, col_in,
          row_out.reshape(1, no), col_out.reshape(nd // LANES, LANES),
          beta_two, rel_step, clip_rms, clip_norm)
        outs = [pltpu.with_memory_space_constraint(o, pltpu.VMEM) for o in outs]
        b_out = [jax.ShapeDtypeStruct(w_in.shape, F32), jax.ShapeDtypeStruct(row_in.shape, F32),
                 jax.ShapeDtypeStruct(col_in.shape, F32), jax.ShapeDtypeStruct(w_out.shape, F32),
                 jax.ShapeDtypeStruct((1, no), F32), jax.ShapeDtypeStruct((nd // LANES, LANES), F32)]
        wi_new, ri_new, ci_new, wo_new, ro_new, co_new = pl.pallas_call(
            update_kernel,
            out_shape=b_out,
            in_specs=[vm] * len(outs),
            out_specs=[hb] * 6,
            scratch_shapes=[pltpu.VMEM((nk * ni // B_IN, B_IN, nff), F32), pltpu.VMEM((nd // CHUNK, no, CHUNK), F32),
                            dma((nk * ni // B_IN,)), dma((nd // CHUNK,)),
                            pltpu.VMEM((nk, ni), F32), pltpu.VMEM((nk, nff), F32), pltpu.VMEM((1, no), F32),
                            pltpu.VMEM((nd // LANES, LANES), F32), dma((4,))],
            compiler_params=pltpu.CompilerParams(vmem_limit_bytes=SCOPED),
            name="update",
        )(*outs)
        return (wi_new, ri_new, ci_new, wo_new, ro_new.reshape(no), co_new.reshape(nd))

    in_specs = (P(None, 'tp'), P(None, 'tp'), P(), P(), P(None, 'tp', None), P('tp', None),
                P(None, 'tp'), P(), P('tp'), P(), P(), P(), P(), P())
    out_specs = (P(None, 'tp', None), P(None, 'tp'), P(), P('tp', None), P('tp'), P())
    return jax.shard_map(local_step, mesh=mesh, in_specs=in_specs, out_specs=out_specs, check_vma=False)
```
